32 devices in a mesh: blk: 16 (over z, x, core), dp: 2 (over y).
Axes of the slice: x: 2, y: 2, z: 4, core: 2. Of those that a mesh axis runs over, the one named last changes fastest.
Arguments:
- inputs: bfloat16 [4096, 1024], P(('blk', 'dp')), may hold values from -6 to 6
- cotangent: bfloat16 [4096, 1024], P(('blk', 'dp')), may hold values from -2.5 to 2.5
- task_ids: int32 [4096], P(('blk', 'dp')), may hold values from 0 to 3
- group_counts: int32 [32, 8], P(('blk', 'dp')), may hold values from 1 to 16, as said below
- task_gate: float32 [4, 16], replicated, may hold values from 0.25 to 2
- w_in: bfloat16 [16, 1024, 2048], P('blk'), may hold values from -0.1875 to 0.1875
- w_out: bfloat16 [16, 2048, 1024], P('blk'), may hold values from -0.125 to 0.125
Outputs:
- input_grad: float32 [4096, 1024], P(('blk', 'dp'))
- grad_in: float32 [16, 1024, 2048], P('blk', 'dp')
- grad_out: float32 [16, 2048, 1024], P('blk', 'dp')
The draws below stay inside these ranges and needn't reach their ends.
Inputs may be any that keep to these rules, and one draw needn't show every extreme that they name: `group_counts`: in every draw one group has all 16 slots live on every device; the others vary from device to device.
All inputs are finite; a program needn't handle non-finite values.
Results may differ from the reference program's by a relative error of at most 0.0042.
Values may be sent and summed in bfloat16 or wider, within the bound.
A program may use at most 128 MiB of HBM per device.

```python
import math
import jax
import jax.numpy as jnp
from jax import lax

D = 1024
HW = 2048
GROUPS = 8
TASKS = 4
CAP = 16
EXPERTS = 16
SOURCES = 32
SAMPLES = 4096


def draw_group_counts(key, part):
    key_level = jax.random.fold_in(key, 11)
    key_raw = jax.random.fold_in(key, 12)
    key_full = jax.random.fold_in(key, 13)
    level = jax.random.randint(key_level, (GROUPS,), max(1, CAP // 4), CAP + 1)
    raw_values = jax.random.randint(key_raw, (SOURCES, GROUPS), 0, 1 << 20)
    counts = 1 + raw_values % level[None, :]
    full_group = jax.random.randint(key_full, (), 0, GROUPS)
    filled = jnp.where(jnp.arange(GROUPS)[None, :] == full_group, CAP, counts)
    return filled.astype(jnp.int32)


def with_ends(entries, rng, smallest, high):
    longest = entries.shape.index(max(entries.shape))
    spots = []
    for shift in (0, 1):
        where = [jax.random.randint(jax.random.fold_in(rng, axis), (), 0, length) for axis, length in enumerate(entries.shape)]
        where[longest] = (where[longest] + shift) % entries.shape[longest]
        spots.append(tuple(where))
    return entries.at[spots[0]].set(smallest).at[spots[1]].set(high)


def level_of(stream_key, dims, cuts, least, high):
    loudness = 1.0
    for dim, shards_of in cuts:
        steps = jax.random.uniform(jax.random.fold_in(jax.random.fold_in(stream_key, 6), dim), (shards_of,), jnp.float32, least / len(cuts), high / len(cuts))
        loudness = loudness * jnp.repeat(jnp.exp(steps), dims[dim] // shards_of).reshape((-1,) + (1,) * (len(dims) - 1 - dim))
    return loudness


def noise(key, dims, deviation, limit, shards=(), kind=jnp.bfloat16):
    level = level_of(key, dims, shards, -0.22, 0.18) if shards else 1.0
    drawn = jax.random.normal(key, dims, jnp.float32) * deviation * level
    return jnp.minimum(jnp.maximum(drawn, -limit), limit).astype(kind)


def setup_inputs(seed: int = 0) -> dict:
    key_list = jax.random.split(jax.random.key(seed), 8)
    return {
        "inputs": noise(key_list[0], (SAMPLES, D), 1.0, 6.0, ((0, 32),)),
        "cotangent": noise(key_list[1], (SAMPLES, D), 0.35, 2.5, ((0, 32),)),
        "task_ids": with_ends(jax.random.randint(key_list[2], (SAMPLES,), 0, TASKS), jax.random.fold_in(key_list[2], 1), 0, TASKS - 1).astype(jnp.int32),
        "group_counts": draw_group_counts(jax.random.fold_in(key_list[7], 71), 0),
        "task_gate": jnp.clip(jnp.exp(jax.random.uniform(key_list[4], (TASKS, EXPERTS), jnp.float32, math.log(0.25), math.log(2.0))), 0.25, 2.0),
        "w_in": noise(key_list[5], (EXPERTS, D, HW), D ** -0.5, 0.1875, ((0, 16),)),
        "w_out": noise(key_list[6], (EXPERTS, HW, D), HW ** -0.5, 0.125, ((0, 16),)),
    }


grad_scale = 0.0625


def reference(inputs, cotangent, task_ids, group_counts, task_gate, w_in, w_out):
    inputs_four = inputs.reshape(SOURCES, GROUPS, CAP, D)
    cot_four = cotangent.reshape(SOURCES, GROUPS, CAP, D)
    task_three = task_ids.reshape(SOURCES, GROUPS, CAP)
    slot_index = jnp.arange(CAP, dtype=jnp.int32)
    live_three = slot_index[None, None, :] < group_counts[:, :, None]

    def per_expert(accum, expert):
        group = (expert % GROUPS).astype(jnp.int32)
        x_rows = lax.dynamic_index_in_dim(inputs_four, group, 1, keepdims=False).reshape(SOURCES * CAP, D)
        cot_rows = lax.dynamic_index_in_dim(cot_four, group, 1, keepdims=False).reshape(SOURCES * CAP, D)
        task_rows = lax.dynamic_index_in_dim(task_three, group, 1, keepdims=False).reshape(SOURCES * CAP)
        live_rows = lax.dynamic_index_in_dim(live_three, group, 1, keepdims=False).reshape(SOURCES * CAP)
        column = lax.dynamic_index_in_dim(task_gate, expert.astype(jnp.int32), 1, keepdims=False)
        row_gate = jnp.where(live_rows, column[task_rows], jnp.zeros((), task_gate.dtype)).astype(jnp.float32)
        first_weight = lax.dynamic_index_in_dim(w_in, expert.astype(jnp.int32), 0, keepdims=False)
        second_weight = lax.dynamic_index_in_dim(w_out, expert.astype(jnp.int32), 0, keepdims=False)
        pre_act = jnp.dot(x_rows, first_weight, preferred_element_type=jnp.float32)
        sigmoid_act = jax.nn.sigmoid(pre_act)
        hidden = (pre_act * sigmoid_act).astype(jnp.bfloat16)
        scaled_cot = (row_gate[:, None] * cot_rows.astype(jnp.float32)).astype(jnp.bfloat16)
        hidden_cot = jnp.dot(scaled_cot, second_weight.T, preferred_element_type=jnp.float32)
        pre_cot = (hidden_cot * sigmoid_act * (1.0 + pre_act * (1.0 - sigmoid_act))).astype(jnp.bfloat16)
        grad_second = jnp.dot(hidden.T, scaled_cot, preferred_element_type=jnp.float32) * grad_scale
        grad_first = jnp.dot(x_rows.T, pre_cot, preferred_element_type=jnp.float32) * grad_scale
        row_grad = jnp.dot(pre_cot, first_weight.T, preferred_element_type=jnp.float32)
        current = lax.dynamic_index_in_dim(accum, group, 1, keepdims=False)
        accum = lax.dynamic_update_index_in_dim(accum, current + row_grad.reshape(SOURCES, CAP, D), group, 1)
        return accum, (grad_first, grad_second)

    start = jnp.zeros((SOURCES, GROUPS, CAP, D), jnp.float32)
    accum, stacked = lax.scan(per_expert, start, jnp.arange(EXPERTS, dtype=jnp.int32))
    return accum.reshape(SAMPLES, D), stacked[0], stacked[1]
```

```python
import functools

import jax
import jax.numpy as jnp
from jax import lax
from jax.experimental import pallas as pl
from jax.experimental.pallas import tpu as pltpu
from jax.sharding import PartitionSpec as P

grad_scale = 0.0625
VMEM_BYTES = 46 * 1024 * 1024
MESH = pl.DeviceIdType.MESH


def exchange_kernel(
    n, peers, groups, cap, width, hidden, tasks,
    counts_hbm, gate_hbm, ids_hbm, x_hbm, cot_hbm, w1_hbm, w2_hbm,
    first, second, home,
    counts_ref, gate_ref, ids_ref, cots, tag, pay, buf, w1, w2, ret, xh, sc, act, pc,
    send1, recv1, send2, recv2, send3, recv3, local_sem,
):
    b = lax.axis_index("blk")
    h = lax.axis_index("dp")
    plane = n * cap
    half, quarter = n // 2, n // 4
    early = n - quarter
    width_part = width // peers
    hidden_part = hidden // peers
    tile = 512
    tiles = hidden // tile
    part_tiles = hidden_part // tile
    side, place = b // half, lax.rem(b, half)
    step, spot = place // quarter, lax.rem(place, quarter)

    def device_at(z, shift):
        return z * quarter + lax.rem(spot + shift, quarter)

    def near_target(i):
        return device_at(2 * side + step, quarter - i)

    def cross_target(i):
        return device_at(2 * side + 1 - step, quarter - i)

    def far_target(i):
        return device_at(2 - 2 * side + lax.rem(i, 2), quarter - i // 2)

    def far_slot(i):
        return (1 + 2 * lax.rem(side + step, 2)) * quarter + i // 2

    def near_source(i):
        return device_at(2 * side + step, i)

    def outer_source(i):
        return device_at(3 - 3 * side, i)

    def cross_source(i):
        return device_at(2 * side + 1 - step, i)

    def inner_source(i):
        return device_at(2 - side, i)

    def slot_rows(i):
        return pl.ds(pl.multiple_of(i * cap, cap), cap)

    barrier = pltpu.get_barrier_semaphore()

    @pl.loop(1, n)
    def _(k):
        pl.semaphore_signal(barrier, inc=1, device_id=(lax.rem(b + k, n), h), device_id_type=MESH)

    for j in range(1, peers):
        pl.semaphore_signal(barrier, inc=1, device_id=(b, lax.rem(h + j, peers)), device_id_type=MESH)

    loads = [
        pltpu.make_async_copy(source, target, local_sem.at[6 + at])
        for at, (source, target) in enumerate(
            [(counts_hbm, counts_ref), (gate_hbm, gate_ref), (ids_hbm, ids_ref), (cot_hbm, cots)]
            + [(x_hbm, pay.at[pl.ds(r * groups, groups), :, pl.ds(0, width)]) for r in range(n // groups)]
        )
    ]
    for load in loads:
        load.start()
    get_w1 = pltpu.make_async_copy(w1_hbm.at[0], w1, local_sem.at[3])
    get_w2 = pltpu.make_async_copy(w2_hbm.at[0], w2, local_sem.at[4])
    get_w1.start()
    get_w2.start()
    for load in loads[:4]:
        load.wait()
    slots = groups * cap
    lanes = lax.broadcasted_iota(jnp.int32, (slots, slots), 1)
    places = lax.broadcasted_iota(jnp.int32, (slots, slots), 0)
    ids = jnp.broadcast_to(ids_ref[...].astype(jnp.float32), (slots, slots))
    tag[...] = jnp.broadcast_to(
        jnp.sum(jnp.where(lanes == places, ids, 0.0), axis=1, keepdims=True), tag.shape
    )
    order = lax.broadcasted_iota(jnp.int32, (cap, 1), 0)

    @pl.loop(0, groups)
    def _(g):
        known = tag[slot_rows(g), :][:, 0:1]
        live = order < counts_ref[0, g]
        cot_rows = cots[g].astype(jnp.float32)
        for r in range(n // groups):
            gate = jnp.zeros((cap, 1), jnp.float32)
            for t in range(tasks):
                gate = jnp.where(known == float(t), gate_ref[t, r * groups + g], gate)
            gate = jnp.where(live, gate, 0.0)
            pay[r * groups + g, :, pl.ds(width, width)] = (gate * cot_rows).astype(jnp.bfloat16)

    for load in loads[4:]:
        load.wait()
    own = pltpu.make_async_copy(pay.at[b], buf.at[0, pl.ds(0, cap)], local_sem.at[2])
    own.start()
    pl.semaphore_wait(barrier, n - 1 + peers - 1)

    def block_out(target, at, slot):
        return pltpu.make_async_remote_copy(
            src_ref=pay.at[target], dst_ref=buf.at[0, slot_rows(slot)],
            send_sem=send1.at[at], recv_sem=recv1.at[slot],
            device_id=(target, h), device_id_type=MESH,
        )

    def forward(i, j):
        return pltpu.make_async_remote_copy(
            src_ref=buf.at[0, slot_rows(i)], dst_ref=buf.at[j, slot_rows(i)],
            send_sem=send2.at[j - 1, i], recv_sem=recv2.at[j - 1, i],
            device_id=(b, lax.rem(h + j, peers)), device_id_type=MESH,
        )

    def own_across(j):
        return pltpu.make_async_remote_copy(
            src_ref=pay.at[b], dst_ref=buf.at[j, slot_rows(0)],
            send_sem=send2.at[j - 1, 0], recv_sem=recv2.at[j - 1, 0],
            device_id=(b, lax.rem(h + j, peers)), device_id_type=MESH,
        )

    def homeward(i, target):
        return pltpu.make_async_remote_copy(
            src_ref=ret.at[slot_rows(i)], dst_ref=home.at[b],
            send_sem=send3.at[i], recv_sem=recv3.at[b],
            device_id=(target, h), device_id_type=MESH,
        )

    def home_from(source):
        return pltpu.make_async_remote_copy(
            src_ref=ret.at[slot_rows(0)], dst_ref=home.at[source],
            send_sem=send3.at[0], recv_sem=recv3.at[source],
            device_id=(source, h), device_id_type=MESH,
        )

    def pass_on(i):
        block_out(b, i, i).wait_recv()
        for j in range(1, peers):
            forward(i, j).start()

    @pl.loop(0, half)
    def _(i):
        block_out(far_target(i), half + i, far_slot(i)).start()

    @pl.loop(1, quarter)
    def _(i):
        block_out(near_target(i), i, i).start()

    @pl.loop(0, quarter)
    def _(i):
        block_out(cross_target(i), quarter + i, half + i).start()

    for j in range(1, peers):
        own_across(j).start()

    @pl.loop(1, half)
    def _(i):
        pass_on(i)

    own.wait()
    get_w1.wait()
    get_w2.wait()

    def rows_forward(j, slot, count):
        start, total = slot * cap, count * cap
        rows = pl.ds(start, total)
        flat = pl.ds((slot // half * peers + j) * half * cap, total)
        sc[flat, :] = buf[j, rows, pl.ds(width, width)]
        xh[flat, :] = buf[j, rows, pl.ds(pl.multiple_of(h * width_part, width_part), width_part)]

        def hidden_tile(q, keep):
            at = lax.rem(h * hidden_part + q * tile, hidden)
            columns = pl.ds(pl.multiple_of(at, tile), tile)
            pre = jnp.dot(
                buf[j, rows, pl.ds(0, width)], w1[:, columns], preferred_element_type=jnp.float32
            )
            sig = jax.nn.sigmoid(pre)
            if keep:
                act[flat, pl.ds(pl.multiple_of(q * tile, tile), tile)] = (pre * sig).astype(jnp.bfloat16)
            cot = lax.dot_general(
                buf[j, rows, pl.ds(width, width)], w2[columns, :], (((1,), (1,)), ((), ())), preferred_element_type=jnp.float32
            )
            pc[flat, columns] = (cot * (sig * (1.0 + pre * (1.0 - sig)))).astype(jnp.bfloat16)

        @pl.loop(0, part_tiles)
        def _(q):
            hidden_tile(q, True)

        @pl.loop(part_tiles, tiles)
        def _(q):
            hidden_tile(q, False)

    def rows_home(slot, count):
        rows = pl.ds(slot * cap, count * cap)
        flat = pl.ds(slot * peers * cap, count * cap)

        @pl.loop(0, width // tile)
        def _(d):
            columns = pl.ds(pl.multiple_of(d * tile, tile), tile)
            grad = lax.dot_general(
                pc[flat, :], w1[columns, :], (((1,), (1,)), ((), ())), preferred_element_type=jnp.float32
            )
            ret[rows, columns] = grad.astype(jnp.bfloat16)

    def partner_rows(j, start, count):
        @pl.loop(start, start + count)
        def _(i):
            forward(i, j).wait_recv()
        rows_forward(j, start, count)

    turned = (((0,), (0,)), ((), ()))
    chunk = peers * half * cap

    def grads(part):
        rows = pl.ds(part * chunk, chunk)

        def add(out, columns, left, right):
            grad = lax.dot_general(left, right, turned, preferred_element_type=jnp.float32)
            if part:
                grad = (out[:, columns] + grad) * grad_scale
            out[:, columns] = grad

        @pl.loop(0, tiles)
        def _(q):
            columns = pl.ds(pl.multiple_of(q * tile, tile), tile)
            add(first, columns, xh[rows, :], pc[rows, columns])

        @pl.loop(0, width // tile)
        def _(q):
            columns = pl.ds(pl.multiple_of(q * tile, tile), tile)
            add(second, columns, act[rows, :], sc[rows, columns])

    rows_forward(0, 0, half)
    rows_home(0, half)
    own_home = pltpu.make_async_copy(ret.at[pl.ds(0, cap)], home.at[b], local_sem.at[5])
    own_home.start()

    @pl.loop(1, quarter)
    def _(i):
        homeward(i, near_source(i)).start()

    middle = early + quarter // 2

    @pl.loop(half, middle)
    def _(i):
        pass_on(i)

    for j in range(1, peers):
        partner_rows(j, 0, half)

    grads(0)

    @pl.loop(middle, n)
    def _(i):
        pass_on(i)

    @pl.loop(quarter, half)
    def _(i):
        homeward(i, outer_source(i)).start()

    rows_forward(0, half, half)
    rows_home(half, half)

    @pl.loop(early, n)
    def _(i):
        homeward(i, inner_source(i)).start()

    @pl.loop(half, early)
    def _(i):
        homeward(i, cross_source(i)).start()

    for j in range(1, peers):
        partner_rows(j, half, half)

    grads(1)

    own_home.wait()

    @pl.loop(1, n)
    def _(i):
        homeward(i, b).wait_send()

    @pl.loop(1, n)
    def _(i):
        block_out(b, i, i).wait_send()

    for j in range(1, peers):
        @pl.loop(0, n)
        def _(i):
            forward(i, j).wait_send()

    @pl.loop(1, n)
    def _(k):
        home_from(lax.rem(b + k, n)).wait_recv()


def finish_kernel(first, second, home, out_rows, out_first, out_second, rows, sem):
    put_first = pltpu.make_async_copy(first, out_first.at[0], sem.at[0])
    put_second = pltpu.make_async_copy(second, out_second.at[0], sem.at[1])
    put_first.start()
    put_second.start()
    repeats, total = home.shape[0], jnp.float32(0.0)
    for r in range(repeats):
        total = total + home[r].astype(jnp.float32)
    rows[...] = total
    put_rows = pltpu.make_async_copy(rows, out_rows, sem.at[2])
    put_rows.start()
    put_first.wait()
    put_second.wait()
    put_rows.wait()


def on_device(n, peers, inputs, cotangent, task_ids, group_counts, task_gate, w_in, w_out):
    groups = group_counts.shape[1]
    slots, width = inputs.shape
    hidden = w_in.shape[2]
    cap = slots // groups
    tasks = task_gate.shape[0]
    rows = peers * n * cap
    bf16 = jnp.bfloat16
    hbm = pl.BlockSpec(memory_space=pltpu.HBM)
    vmem = pl.BlockSpec(memory_space=pltpu.VMEM)
    dma = pltpu.SemaphoreType.DMA
    first, second, home = pl.pallas_call(
        functools.partial(exchange_kernel, n, peers, groups, cap, width, hidden, tasks),
        out_shape=(
            pltpu.VMEM((width // peers, hidden), jnp.float32),
            pltpu.VMEM((hidden // peers, width), jnp.float32),
            pltpu.VMEM((n, cap, width), bf16),
        ),
        in_specs=[hbm] * 7,
        out_specs=(vmem,) * 3,
        scratch_shapes=[
            pltpu.SMEM(group_counts.shape, jnp.int32),
            pltpu.SMEM(task_gate.shape, jnp.float32),
            pltpu.VMEM((1, slots), jnp.int32),
            pltpu.VMEM((groups, cap, width), bf16),
            pltpu.VMEM((slots, slots), jnp.float32),
            pltpu.VMEM((n, cap, 2 * width), bf16),
            pltpu.VMEM((peers, n * cap, 2 * width), bf16),
            pltpu.VMEM((width, hidden), bf16),
            pltpu.VMEM((hidden, width), bf16),
            pltpu.VMEM((n * cap, width), bf16),
            pltpu.VMEM((rows, width // peers), bf16),
            pltpu.VMEM((rows, width), bf16),
            pltpu.VMEM((rows, hidden // peers), bf16),
            pltpu.VMEM((rows, hidden), bf16),
            dma((n,)), dma((n,)), dma((peers - 1, n)), dma((peers - 1, n)), dma((n,)), dma((n,)),
            dma((10 + n // groups,)),
        ],
        compiler_params=pltpu.CompilerParams(
            collective_id=0, has_side_effects=True, vmem_limit_bytes=VMEM_BYTES
        ),
    )(
        *(
            pltpu.with_memory_space_constraint(array, pltpu.HBM)
            for array in (
                group_counts, task_gate, task_ids.reshape(1, slots), inputs.reshape(groups, cap, width),
                cotangent.reshape(groups, cap, width), w_in, w_out,
            )
        )
    )
    return pl.pallas_call(
        finish_kernel,
        out_shape=(
            jax.ShapeDtypeStruct((slots, width), jnp.float32),
            jax.ShapeDtypeStruct((1,) + first.shape, jnp.float32),
            jax.ShapeDtypeStruct((1,) + second.shape, jnp.float32),
        ),
        in_specs=[vmem] * 3,
        out_specs=(hbm,) * 3,
        scratch_shapes=[pltpu.VMEM((slots, width), jnp.float32), dma((3,))],
        compiler_params=pltpu.CompilerParams(vmem_limit_bytes=4 * 1024 * 1024),
    )(first, second, home.reshape(n // groups, slots, width))


def solution(mesh):
    in_specs = (
        P(("blk", "dp"), None),
        P(("blk", "dp"), None),
        P(("blk", "dp")),
        P(("blk", "dp"), None),
        P(),
        P("blk", None, None),
        P("blk", None, None),
    )
    out_specs = (P(("blk", "dp"), None), P("blk", "dp", None), P("blk", "dp", None))
    body = functools.partial(on_device, mesh.shape["blk"], mesh.shape["dp"])
    return jax.shard_map(body, mesh=mesh, in_specs=in_specs, out_specs=out_specs, check_vma=False)
```

```python
import functools

import jax
import jax.numpy as jnp
from jax import lax
from jax.experimental import pallas as pl
from jax.experimental.pallas import tpu as pltpu
from jax.sharding import PartitionSpec as P

grad_scale = 0.0625
VMEM_BYTES = 46 * 1024 * 1024
PIECES = 4
RELEASE = 1
MESH = pl.DeviceIdType.MESH


def exchange_kernel(
    n, peers, groups, cap, width, hidden, tasks,
    counts_hbm, gate_hbm, ids_hbm, x_hbm, cot_hbm, w1_hbm, w2_hbm,
    first, second, home,
    counts_ref, gate_ref, ids_ref, cots, tag, pay, buf, w1, w2, ret, xh, sc, act, pc,
    send1, recv1, send2, recv2, send3, recv3, local_sem,
):
    b = lax.axis_index("blk")
    h = lax.axis_index("dp")
    plane = n * cap
    half, quarter = n // 2, n // 4
    early = n - quarter
    width_part = width // peers
    hidden_part = hidden // peers
    tile = 512
    tiles = hidden // tile
    part_tiles = hidden_part // tile
    side, place = b // half, lax.rem(b, half)
    step, spot = place // quarter, lax.rem(place, quarter)

    def device_at(z, shift):
        return z * quarter + lax.rem(spot + shift, quarter)

    def near_target(i):
        return device_at(2 * side + step, quarter - i)

    def cross_target(i):
        return device_at(2 * side + 1 - step, quarter - i)

    def far_target(i):
        return device_at(2 - 2 * side + lax.rem(i, 2), quarter - i // 2)

    def far_slot(i):
        return (1 + 2 * lax.rem(side + step, 2)) * quarter + i // 2

    def near_source(i):
        return device_at(2 * side + step, i)

    def outer_source(i):
        return device_at(3 - 3 * side, i)

    def cross_source(i):
        return device_at(2 * side + 1 - step, i)

    def inner_source(i):
        return device_at(2 - side, i)

    def slot_rows(i):
        return pl.ds(pl.multiple_of(i * cap, cap), cap)

    barrier = pltpu.get_barrier_semaphore()

    @pl.loop(1, n)
    def _(k):
        pl.semaphore_signal(barrier, inc=1, device_id=(lax.rem(b + k, n), h), device_id_type=MESH)

    for j in range(1, peers):
        @pl.loop(0, quarter)
        def _(i):
            pl.semaphore_signal(
                barrier, inc=1, device_id=(near_target(i), lax.rem(h + j, peers)), device_id_type=MESH
            )

    loads = [
        pltpu.make_async_copy(source, target, local_sem.at[6 + at])
        for at, (source, target) in enumerate(
            [(counts_hbm, counts_ref), (gate_hbm, gate_ref), (ids_hbm, ids_ref), (cot_hbm, cots)]
            + [(x_hbm, pay.at[pl.ds(r * groups, groups), :, pl.ds(0, width)]) for r in range(n // groups)]
        )
    ]
    for load in loads:
        load.start()
    get_w1 = pltpu.make_async_copy(w1_hbm.at[0], w1, local_sem.at[3])
    get_w2 = pltpu.make_async_copy(w2_hbm.at[0], w2, local_sem.at[4])
    get_w1.start()
    get_w2.start()
    for load in loads[:4]:
        load.wait()
    slots = groups * cap
    lanes = lax.broadcasted_iota(jnp.int32, (slots, slots), 1)
    places = lax.broadcasted_iota(jnp.int32, (slots, slots), 0)
    ids = jnp.broadcast_to(ids_ref[...].astype(jnp.float32), (slots, slots))
    tag[...] = jnp.broadcast_to(
        jnp.sum(jnp.where(lanes == places, ids, 0.0), axis=1, keepdims=True), tag.shape
    )
    order = lax.broadcasted_iota(jnp.int32, (cap, 1), 0)

    @pl.loop(0, groups)
    def _(g):
        known = tag[slot_rows(g), :][:, 0:1]
        live = order < counts_ref[0, g]
        cot_rows = cots[g].astype(jnp.float32)
        for r in range(n // groups):
            gate = jnp.zeros((cap, 1), jnp.float32)
            for t in range(tasks):
                gate = jnp.where(known == float(t), gate_ref[t, r * groups + g], gate)
            gate = jnp.where(live, gate, 0.0)
            pay[r * groups + g, :, pl.ds(width, width)] = (gate * cot_rows).astype(jnp.bfloat16)

    for load in loads[4:]:
        load.wait()
    own = pltpu.make_async_copy(pay.at[b], buf.at[0, pl.ds(0, cap)], local_sem.at[2])
    own.start()
    pl.semaphore_wait(barrier, n - 1 + (peers - 1) * quarter)

    def block_out(target, slot):
        return pltpu.make_async_remote_copy(
            src_ref=pay.at[target], dst_ref=buf.at[0, slot_rows(slot)],
            send_sem=send1.at[0], recv_sem=recv1.at[slot],
            device_id=(target, h), device_id_type=MESH,
        )

    def forward(i, j):
        return pltpu.make_async_remote_copy(
            src_ref=buf.at[0, slot_rows(i)], dst_ref=buf.at[j, slot_rows(i)],
            send_sem=send2.at[j - 1], recv_sem=recv2.at[j - 1, i // half],
            device_id=(b, lax.rem(h + j, peers)), device_id_type=MESH,
        )

    def across(i, j):
        target = near_target(i)
        return pltpu.make_async_remote_copy(
            src_ref=pay.at[target], dst_ref=buf.at[j, slot_rows(i)],
            send_sem=send2.at[j - 1], recv_sem=recv2.at[j - 1, i // half],
            device_id=(target, lax.rem(h + j, peers)), device_id_type=MESH,
        )

    def homeward(i, target):
        return pltpu.make_async_remote_copy(
            src_ref=ret.at[slot_rows(i)], dst_ref=home.at[b],
            send_sem=send3.at[0], recv_sem=recv3.at[0],
            device_id=(target, h), device_id_type=MESH,
        )

    def pass_on(i):
        block_out(b, i).wait_recv()
        for j in range(1, peers):
            forward(i, j).start()

    @pl.loop(0, half)
    def _(i):
        block_out(far_target(i), far_slot(i)).start()

    for j in range(1, peers):
        @pl.loop(0, quarter)
        def _(i):
            across(i, j).start()

    @pl.loop(1, quarter)
    def _(i):
        block_out(near_target(i), i).start()

    @pl.loop(0, quarter)
    def _(i):
        block_out(cross_target(i), half + i).start()

    def pass_second(before, after):
        outer = lax.rem(side + step + 1, 2)
        start = before[0] + outer * (before[1] - before[0])
        stop = after[0] + outer * (after[1] - after[0])

        @pl.loop(half + start, half + stop)
        def _(i):
            pass_on(i)

    @pl.loop(quarter, half)
    def _(i):
        pass_on(i)

    points = [(quarter * inner // 4, quarter * outer // 4) for inner, outer in ((0, 0), (0, 4), (2, 5), (3, 6), (6, 7), (8, 8))]
    pass_second(*points[0:2])

    @pl.loop(1, quarter)
    def _(i):
        block_out(b, i).wait_recv()

    own.wait()
    get_w1.wait()
    get_w2.wait()

    def rows_forward(j, slot, count):
        start, total = slot * cap, count * cap
        rows = pl.ds(start, total)
        flat = pl.ds((slot // half * peers + j) * half * cap, total)
        sc[flat, :] = buf[j, rows, pl.ds(width, width)]
        xh[flat, :] = buf[j, rows, pl.ds(pl.multiple_of(h * width_part, width_part), width_part)]

        def hidden_tile(q, keep):
            at = lax.rem(h * hidden_part + q * tile, hidden)
            columns = pl.ds(pl.multiple_of(at, tile), tile)
            pre = jnp.dot(
                buf[j, rows, pl.ds(0, width)], w1[:, columns], preferred_element_type=jnp.float32
            )
            sig = jax.nn.sigmoid(pre)
            if keep:
                act[flat, pl.ds(pl.multiple_of(q * tile, tile), tile)] = (pre * sig).astype(jnp.bfloat16)
            cot = lax.dot_general(
                buf[j, rows, pl.ds(width, width)], w2[columns, :], (((1,), (1,)), ((), ())), preferred_element_type=jnp.float32
            )
            pc[flat, columns] = (cot * (sig * (1.0 + pre * (1.0 - sig)))).astype(jnp.bfloat16)

        @pl.loop(0, part_tiles)
        def _(q):
            hidden_tile(q, True)

        @pl.loop(part_tiles, tiles)
        def _(q):
            hidden_tile(q, False)

    def rows_home(slot, count):
        rows = pl.ds(slot * cap, count * cap)
        flat = pl.ds(slot * peers * cap, count * cap)

        @pl.loop(0, width // tile)
        def _(d):
            columns = pl.ds(pl.multiple_of(d * tile, tile), tile)
            grad = lax.dot_general(
                pc[flat, :], w1[columns, :], (((1,), (1,)), ((), ())), preferred_element_type=jnp.float32
            )
            ret[rows, columns] = grad.astype(jnp.bfloat16)

    def partner_rows(j, start, count):
        rows = buf.at[j, pl.ds(start * cap, count * cap)]
        pltpu.make_async_copy(rows, rows, recv2.at[j - 1, start // half]).wait()
        rows_forward(j, start, count)

    turned = (((0,), (0,)), ((), ()))
    chunk = peers * half * cap

    def grads(part):
        rows = pl.ds(part * chunk, chunk)

        def add(out, columns, left, right):
            grad = lax.dot_general(left, right, turned, preferred_element_type=jnp.float32)
            if part:
                grad = (out[:, columns] + grad) * grad_scale
            out[:, columns] = grad

        @pl.loop(0, tiles)
        def _(q):
            columns = pl.ds(pl.multiple_of(q * tile, tile), tile)
            add(first, columns, xh[rows, :], pc[rows, columns])

        @pl.loop(0, width // tile)
        def _(q):
            columns = pl.ds(pl.multiple_of(q * tile, tile), tile)
            add(second, columns, act[rows, :], sc[rows, columns])

    def release():
        @pl.loop(quarter, half)
        def _(i):
            homeward(i, outer_source(i)).start()

    rows_forward(0, 0, half)
    pass_second(*points[1:3])
    rows_home(0, half)
    own_home = pltpu.make_async_copy(ret.at[pl.ds(0, cap)], home.at[b], local_sem.at[5])
    own_home.start()

    @pl.loop(1, quarter)
    def _(i):
        homeward(i, near_source(i)).start()

    pass_second(*points[2:4])
    for j in range(1, peers):
        partner_rows(j, 0, half)
    pass_second(*points[3:5])
    @pl.when(lax.rem(side + step + 1, 2) < RELEASE)
    def _():
        release()

    grads(0)
    pass_second(*points[4:6])

    @pl.when(lax.rem(side + step + 1, 2) >= RELEASE)
    def _():
        release()


    rows_forward(0, half, half)
    rows_home(half, half)

    @pl.loop(early, n)
    def _(i):
        homeward(i, inner_source(i)).start()

    @pl.loop(half, early)
    def _(i):
        homeward(i, cross_source(i)).start()

    for j in range(1, peers):
        partner_rows(j, half, half)

    grads(1)

    own_home.wait()

    sent = pay.at[pl.ds(0, n - 1)]
    pltpu.make_async_copy(sent, sent, send1.at[0]).wait()
    for j in range(1, peers):
        pltpu.make_async_copy(buf.at[0], buf.at[0], send2.at[j - 1]).wait()
    gone = ret.at[pl.ds(0, (n - 1) * cap)]
    pltpu.make_async_copy(gone, gone, send3.at[0]).wait()

    come = home.at[pl.ds(0, n - 1)]
    pltpu.make_async_copy(come, come, recv3.at[0]).wait()


def finish_kernel(first, second, home, out_rows, out_first, out_second, rows, sem):
    puts = []
    for source, target in ((first, out_first), (second, out_second)):
        step = source.shape[0] // PIECES
        for piece in range(PIECES):
            part = pl.ds(piece * step, step)
            puts.append(pltpu.make_async_copy(source.at[part], target.at[0, part], sem.at[len(puts)]))
            puts[-1].start()
    repeats, total = home.shape[0], jnp.float32(0.0)
    for r in range(repeats):
        total = total + home[r].astype(jnp.float32)
    rows[...] = total
    puts.append(pltpu.make_async_copy(rows, out_rows, sem.at[len(puts)]))
    puts[-1].start()
    for put in puts:
        put.wait()


def on_device(n, peers, inputs, cotangent, task_ids, group_counts, task_gate, w_in, w_out):
    groups = group_counts.shape[1]
    slots, width = inputs.shape
    hidden = w_in.shape[2]
    cap = slots // groups
    tasks = task_gate.shape[0]
    rows = peers * n * cap
    bf16 = jnp.bfloat16
    hbm = pl.BlockSpec(memory_space=pltpu.HBM)
    vmem = pl.BlockSpec(memory_space=pltpu.VMEM)
    dma = pltpu.SemaphoreType.DMA
    first, second, home = pl.pallas_call(
        functools.partial(exchange_kernel, n, peers, groups, cap, width, hidden, tasks),
        out_shape=(
            pltpu.VMEM((width // peers, hidden), jnp.float32),
            pltpu.VMEM((hidden // peers, width), jnp.float32),
            pltpu.VMEM((n, cap, width), bf16),
        ),
        in_specs=[hbm] * 7,
        out_specs=(vmem,) * 3,
        scratch_shapes=[
            pltpu.SMEM(group_counts.shape, jnp.int32),
            pltpu.SMEM(task_gate.shape, jnp.float32),
            pltpu.VMEM((1, slots), jnp.int32),
            pltpu.VMEM((groups, cap, width), bf16),
            pltpu.VMEM((slots, slots), jnp.float32),
            pltpu.VMEM((n, cap, 2 * width), bf16),
            pltpu.VMEM((peers, n * cap, 2 * width), bf16),
            pltpu.VMEM((width, hidden), bf16),
            pltpu.VMEM((hidden, width), bf16),
            pltpu.VMEM((n * cap, width), bf16),
            pltpu.VMEM((rows, width // peers), bf16),
            pltpu.VMEM((rows, width), bf16),
            pltpu.VMEM((rows, hidden // peers), bf16),
            pltpu.VMEM((rows, hidden), bf16),
            dma((1,)), dma((n,)), dma((peers - 1,)), dma((peers - 1, 2)), dma((1,)), dma((1,)),
            dma((10 + n // groups,)),
        ],
        compiler_params=pltpu.CompilerParams(
            collective_id=0, has_side_effects=True, vmem_limit_bytes=VMEM_BYTES
        ),
    )(
        *(
            pltpu.with_memory_space_constraint(array, pltpu.HBM)
            for array in (
                group_counts, task_gate, task_ids.reshape(1, slots), inputs.reshape(groups, cap, width),
                cotangent.reshape(groups, cap, width), w_in, w_out,
            )
        )
    )
    return pl.pallas_call(
        finish_kernel,
        out_shape=(
            jax.ShapeDtypeStruct((slots, width), jnp.float32),
            jax.ShapeDtypeStruct((1,) + first.shape, jnp.float32),
            jax.ShapeDtypeStruct((1,) + second.shape, jnp.float32),
        ),
        in_specs=[vmem] * 3,
        out_specs=(hbm,) * 3,
        scratch_shapes=[pltpu.VMEM((slots, width), jnp.float32), dma((2 * PIECES + 1,))],
        compiler_params=pltpu.CompilerParams(vmem_limit_bytes=4 * 1024 * 1024),
    )(first, second, home.reshape(n // groups, slots, width))


def solution(mesh):
    in_specs = (
        P(("blk", "dp"), None),
        P(("blk", "dp"), None),
        P(("blk", "dp")),
        P(("blk", "dp"), None),
        P(),
        P("blk", None, None),
        P("blk", None, None),
    )
    out_specs = (P(("blk", "dp"), None), P("blk", "dp", None), P("blk", "dp", None))
    body = functools.partial(on_device, mesh.shape["blk"], mesh.shape["dp"])
    return jax.shard_map(body, mesh=mesh, in_specs=in_specs, out_specs=out_specs, check_vma=False)
```

```python
import functools

import jax
import jax.numpy as jnp
from jax import lax
from jax.experimental import pallas as pl
from jax.experimental.pallas import tpu as pltpu
from jax.sharding import PartitionSpec as P

grad_scale = 0.0625
VMEM_BYTES = 46 * 1024 * 1024
PIECES = 4
RELEASE = 1
MESH = pl.DeviceIdType.MESH


def exchange_kernel(
    n, peers, groups, cap, width, hidden, tasks,
    counts_hbm, gate_hbm, ids_hbm, x_hbm, cot_hbm, w1_hbm, w2_hbm,
    first, second, home,
    counts_ref, gate_ref, ids_ref, cots, tag, pay, buf, w1, w2, ret, act, pc,
    send1, recv1, send2, recv2, send3, recv3, local_sem,
):
    b = lax.axis_index("blk")
    h = lax.axis_index("dp")
    half, quarter = n // 2, n // 4
    early = n - quarter
    width_part = width // peers
    hidden_part = hidden // peers
    tile = 512
    tiles = hidden // tile
    part_tiles = hidden_part // tile
    side, place = b // half, lax.rem(b, half)
    step, spot = place // quarter, lax.rem(place, quarter)

    def device_at(z, shift):
        return z * quarter + lax.rem(spot + shift, quarter)

    def near_target(i):
        return device_at(2 * side + step, quarter - i)

    def cross_target(i):
        return device_at(2 * side + 1 - step, quarter - i)

    def far_target(i):
        return device_at(2 - 2 * side + lax.rem(i, 2), quarter - i // 2)

    def far_slot(i):
        return (1 + 2 * lax.rem(side + step, 2)) * quarter + i // 2

    def near_source(i):
        return device_at(2 * side + step, i)

    def outer_source(i):
        return device_at(3 - 3 * side, i)

    def cross_source(i):
        return device_at(2 * side + 1 - step, i)

    def inner_source(i):
        return device_at(2 - side, i)

    def slot_rows(i):
        return pl.ds(pl.multiple_of(i * cap, cap), cap)

    span = half * cap

    def buf_rows(j, i):
        return pl.ds(pl.multiple_of((i // half * peers + j) * span + lax.rem(i, half) * cap, cap), cap)

    barrier = pltpu.get_barrier_semaphore()

    @pl.loop(1, n)
    def _(k):
        pl.semaphore_signal(barrier, inc=1, device_id=(lax.rem(b + k, n), h), device_id_type=MESH)

    for j in range(1, peers):
        @pl.loop(0, quarter)
        def _(i):
            pl.semaphore_signal(
                barrier, inc=1, device_id=(near_target(i), lax.rem(h + j, peers)), device_id_type=MESH
            )

    loads = [
        pltpu.make_async_copy(source, target, local_sem.at[6 + at])
        for at, (source, target) in enumerate(
            [(counts_hbm, counts_ref), (gate_hbm, gate_ref), (ids_hbm, ids_ref), (cot_hbm, cots)]
            + [(x_hbm, pay.at[pl.ds(r * groups, groups), :, pl.ds(0, width)]) for r in range(n // groups)]
        )
    ]
    for load in loads:
        load.start()
    get_w1 = pltpu.make_async_copy(w1_hbm.at[0], w1, local_sem.at[3])
    get_w2 = pltpu.make_async_copy(w2_hbm.at[0], w2, local_sem.at[4])
    get_w1.start()
    get_w2.start()
    for load in loads[:4]:
        load.wait()
    slots = groups * cap
    lanes = lax.broadcasted_iota(jnp.int32, (slots, slots), 1)
    places = lax.broadcasted_iota(jnp.int32, (slots, slots), 0)
    ids = jnp.broadcast_to(ids_ref[...].astype(jnp.float32), (slots, slots))
    tag[...] = jnp.broadcast_to(
        jnp.sum(jnp.where(lanes == places, ids, 0.0), axis=1, keepdims=True), tag.shape
    )
    order = lax.broadcasted_iota(jnp.int32, (cap, 1), 0)

    @pl.loop(0, groups)
    def _(g):
        known = tag[slot_rows(g), :][:, 0:1]
        live = order < counts_ref[0, g]
        cot_rows = cots[g].astype(jnp.float32)
        for r in range(n // groups):
            gate = jnp.zeros((cap, 1), jnp.float32)
            for t in range(tasks):
                gate = jnp.where(known == float(t), gate_ref[t, r * groups + g], gate)
            gate = jnp.where(live, gate, 0.0)
            pay[r * groups + g, :, pl.ds(width, width)] = (gate * cot_rows).astype(jnp.bfloat16)

    for load in loads[4:]:
        load.wait()
    own = pltpu.make_async_copy(pay.at[b], buf.at[pl.ds(0, cap)], local_sem.at[2])
    own.start()
    pl.semaphore_wait(barrier, n - 1 + (peers - 1) * quarter)

    def block_out(target, slot):
        return pltpu.make_async_remote_copy(
            src_ref=pay.at[target], dst_ref=buf.at[buf_rows(0, slot)],
            send_sem=send1.at[0], recv_sem=recv1.at[slot],
            device_id=(target, h), device_id_type=MESH,
        )

    def forward(i, j):
        return pltpu.make_async_remote_copy(
            src_ref=buf.at[buf_rows(0, i)], dst_ref=buf.at[buf_rows(j, i)],
            send_sem=send2.at[j - 1], recv_sem=recv2.at[j - 1, i // half],
            device_id=(b, lax.rem(h + j, peers)), device_id_type=MESH,
        )

    def across(i, j):
        target = near_target(i)
        return pltpu.make_async_remote_copy(
            src_ref=pay.at[target], dst_ref=buf.at[buf_rows(j, i)],
            send_sem=send2.at[j - 1], recv_sem=recv2.at[j - 1, i // half],
            device_id=(target, lax.rem(h + j, peers)), device_id_type=MESH,
        )

    def homeward(i, target):
        return pltpu.make_async_remote_copy(
            src_ref=ret.at[slot_rows(i)], dst_ref=home.at[b],
            send_sem=send3.at[0], recv_sem=recv3.at[0],
            device_id=(target, h), device_id_type=MESH,
        )

    def pass_on(i):
        block_out(b, i).wait_recv()
        for j in range(1, peers):
            forward(i, j).start()

    @pl.loop(0, half)
    def _(i):
        block_out(far_target(i), far_slot(i)).start()

    for j in range(1, peers):
        @pl.loop(0, quarter)
        def _(i):
            across(i, j).start()

    @pl.loop(1, quarter)
    def _(i):
        block_out(near_target(i), i).start()

    @pl.loop(0, quarter)
    def _(i):
        block_out(cross_target(i), half + i).start()

    def pass_second(before, after):
        outer = lax.rem(side + step + 1, 2)
        start = before[0] + outer * (before[1] - before[0])
        stop = after[0] + outer * (after[1] - after[0])

        @pl.loop(half + start, half + stop)
        def _(i):
            pass_on(i)

    @pl.loop(quarter, half)
    def _(i):
        pass_on(i)

    points = [
        (quarter * inner // 4, quarter * outer // 4)
        for inner, outer in ((0, 0), (0, 4), (1, 5), (2, 5), (2, 6), (3, 6), (6, 6), (7, 7), (8, 8))
    ]
    met = []

    def poll(wanted=True):
        if wanted:
            met.append(0)
            pass_second(*points[len(met) - 1:len(met) + 1])

    poll()

    @pl.loop(1, quarter)
    def _(i):
        block_out(b, i).wait_recv()

    own.wait()
    get_w1.wait()
    get_w2.wait()

    def rows_forward(start, total, hook=lambda q: None):
        rows = pl.ds(start, total)

        def hidden_tile(q):
            at = lax.rem(h * hidden_part + q * tile, hidden)
            columns = pl.ds(pl.multiple_of(at, tile), tile)
            pre = jnp.dot(
                buf[rows, pl.ds(0, width)], w1[:, columns], preferred_element_type=jnp.float32
            )
            sig = jax.nn.sigmoid(pre)
            if q < part_tiles:
                act[rows, pl.ds(q * tile, tile)] = (pre * sig).astype(jnp.bfloat16)
            cot = lax.dot_general(
                buf[rows, pl.ds(width, width)], w2[columns, :], (((1,), (1,)), ((), ())), preferred_element_type=jnp.float32
            )
            pc[rows, columns] = (cot * (sig * (1.0 + pre * (1.0 - sig)))).astype(jnp.bfloat16)

        for q in range(tiles):
            hidden_tile(q)
            hook(q)

    def rows_home(part, hook=lambda d: None):
        rows = pl.ds(part * span, span)
        flat = pl.ds(part * peers * span, span)

        for d in range(width // tile):
            columns = pl.ds(d * tile, tile)
            grad = lax.dot_general(
                pc[flat, :], w1[columns, :], (((1,), (1,)), ((), ())), preferred_element_type=jnp.float32
            )
            ret[rows, columns] = grad.astype(jnp.bfloat16)
            hook(d)

    def partner_come(part):
        for j in range(1, peers):
            rows = buf.at[pl.ds((part * peers + j) * span, span)]
            pltpu.make_async_copy(rows, rows, recv2.at[j - 1, part]).wait()

    turned = (((0,), (0,)), ((), ()))
    chunk = peers * span

    def grads(part, hook=lambda: None):
        rows = pl.ds(part * chunk, chunk)

        def add(out, columns, left, right):
            grad = lax.dot_general(left, right, turned, preferred_element_type=jnp.float32)
            if part:
                grad = (out[:, columns] + grad) * grad_scale
            out[:, columns] = grad

        for q in range(tiles):
            columns = pl.ds(q * tile, tile)
            add(first, columns, buf[rows, pl.ds(pl.multiple_of(h * width_part, width_part), width_part)], pc[rows, columns])
        hook()
        for q in range(width // tile):
            columns = pl.ds(q * tile, tile)
            add(second, columns, act[rows, :], buf[rows, pl.ds(width + q * tile, tile)])

    def release():
        @pl.loop(quarter, half)
        def _(i):
            homeward(i, outer_source(i)).start()

    rows_forward(0, span)
    poll()
    rows_home(0, lambda d: poll(d == 0))
    own_home = pltpu.make_async_copy(ret.at[pl.ds(0, cap)], home.at[b], local_sem.at[5])
    own_home.start()

    @pl.loop(1, quarter)
    def _(i):
        homeward(i, near_source(i)).start()

    poll()
    partner_come(0)
    rows_forward(span, chunk - span, lambda q: poll(2 * (q + 1) == tiles))
    poll()
    @pl.when(lax.rem(side + step + 1, 2) < RELEASE)
    def _():
        release()

    grads(0, poll)
    poll()

    @pl.when(lax.rem(side + step + 1, 2) >= RELEASE)
    def _():
        release()


    rows_forward(chunk, span)
    rows_home(1)

    @pl.loop(early, n)
    def _(i):
        homeward(i, inner_source(i)).start()

    @pl.loop(half, early)
    def _(i):
        homeward(i, cross_source(i)).start()

    partner_come(1)
    rows_forward(chunk + span, chunk - span)

    grads(1)

    own_home.wait()

    sent = pay.at[pl.ds(0, n - 1)]
    pltpu.make_async_copy(sent, sent, send1.at[0]).wait()
    for j in range(1, peers):
        whole = buf.at[pl.ds(0, 2 * span)]
        pltpu.make_async_copy(whole, whole, send2.at[j - 1]).wait()
    gone = ret.at[pl.ds(0, (n - 1) * cap)]
    pltpu.make_async_copy(gone, gone, send3.at[0]).wait()

    come = home.at[pl.ds(0, n - 1)]
    pltpu.make_async_copy(come, come, recv3.at[0]).wait()


def finish_kernel(first, second, home, out_rows, out_first, out_second, rows, sem):
    puts = []
    for source, target in ((first, out_first), (second, out_second)):
        step = source.shape[0] // PIECES
        for piece in range(PIECES):
            part = pl.ds(piece * step, step)
            puts.append(pltpu.make_async_copy(source.at[part], target.at[0, part], sem.at[len(puts)]))
            puts[-1].start()
    repeats, total = home.shape[0], jnp.float32(0.0)
    for r in range(repeats):
        total = total + home[r].astype(jnp.float32)
    rows[...] = total
    puts.append(pltpu.make_async_copy(rows, out_rows, sem.at[len(puts)]))
    puts[-1].start()
    for put in puts:
        put.wait()


def on_device(n, peers, inputs, cotangent, task_ids, group_counts, task_gate, w_in, w_out):
    groups = group_counts.shape[1]
    slots, width = inputs.shape
    hidden = w_in.shape[2]
    cap = slots // groups
    tasks = task_gate.shape[0]
    rows = peers * n * cap
    bf16 = jnp.bfloat16
    hbm = pl.BlockSpec(memory_space=pltpu.HBM)
    vmem = pl.BlockSpec(memory_space=pltpu.VMEM)
    dma = pltpu.SemaphoreType.DMA
    first, second, home = pl.pallas_call(
        functools.partial(exchange_kernel, n, peers, groups, cap, width, hidden, tasks),
        out_shape=(
            pltpu.VMEM((width // peers, hidden), jnp.float32),
            pltpu.VMEM((hidden // peers, width), jnp.float32),
            pltpu.VMEM((n, cap, width), bf16),
        ),
        in_specs=[hbm] * 7,
        out_specs=(vmem,) * 3,
        scratch_shapes=[
            pltpu.SMEM(group_counts.shape, jnp.int32),
            pltpu.SMEM(task_gate.shape, jnp.float32),
            pltpu.VMEM((1, slots), jnp.int32),
            pltpu.VMEM((groups, cap, width), bf16),
            pltpu.VMEM((slots, slots), jnp.float32),
            pltpu.VMEM((n, cap, 2 * width), bf16),
            pltpu.VMEM((rows, 2 * width), bf16),
            pltpu.VMEM((width, hidden), bf16),
            pltpu.VMEM((hidden, width), bf16),
            pltpu.VMEM((n * cap, width), bf16),
            pltpu.VMEM((rows, hidden // peers), bf16),
            pltpu.VMEM((rows, hidden), bf16),
            dma((1,)), dma((n,)), dma((peers - 1,)), dma((peers - 1, 2)), dma((1,)), dma((1,)),
            dma((10 + n // groups,)),
        ],
        compiler_params=pltpu.CompilerParams(
            collective_id=0, has_side_effects=True, vmem_limit_bytes=VMEM_BYTES
        ),
    )(
        *(
            pltpu.with_memory_space_constraint(array, pltpu.HBM)
            for array in (
                group_counts, task_gate, task_ids.reshape(1, slots), inputs.reshape(groups, cap, width),
                cotangent.reshape(groups, cap, width), w_in, w_out,
            )
        )
    )
    return pl.pallas_call(
        finish_kernel,
        out_shape=(
            jax.ShapeDtypeStruct((slots, width), jnp.float32),
            jax.ShapeDtypeStruct((1,) + first.shape, jnp.float32),
            jax.ShapeDtypeStruct((1,) + second.shape, jnp.float32),
        ),
        in_specs=[vmem] * 3,
        out_specs=(hbm,) * 3,
        scratch_shapes=[pltpu.VMEM((slots, width), jnp.float32), dma((2 * PIECES + 1,))],
        compiler_params=pltpu.CompilerParams(vmem_limit_bytes=4 * 1024 * 1024),
    )(first, second, home.reshape(n // groups, slots, width))


def solution(mesh):
    in_specs = (
        P(("blk", "dp"), None),
        P(("blk", "dp"), None),
        P(("blk", "dp")),
        P(("blk", "dp"), None),
        P(),
        P("blk", None, None),
        P("blk", None, None),
    )
    out_specs = (P(("blk", "dp"), None), P("blk", "dp", None), P("blk", "dp", None))
    body = functools.partial(on_device, mesh.shape["blk"], mesh.shape["dp"])
    return jax.shard_map(body, mesh=mesh, in_specs=in_specs, out_specs=out_specs, check_vma=False)
```

```python
import functools

import jax
import jax.numpy as jnp
from jax import lax
from jax.experimental import pallas as pl
from jax.experimental.pallas import tpu as pltpu
from jax.sharding import PartitionSpec as P

grad_scale = 0.0625
VMEM_BYTES = 51 * 1024 * 1024
PIECES = 4
RELEASE = (2, 2, 2, 1)
tile = 512
SCHEDULE = (
    (((0, 4), (0, 0), (0, 0), (0, 4)),),
    (((0, 0), (0, 1), (0, 0), (0, 0)),),
    (((0, 0), (1, 2), (0, 0), (0, 0)),),
    (((4, 6), (0, 0), (4, 6), (4, 5)),),
    (((0, 0), (2, 3), (0, 0), (0, 0)),),
    (((0, 0), (3, 6), (0, 2), (5, 6)),),
    (((6, 7), (6, 7), (0, 0), (6, 7)),),
    (((7, 8), (7, 8), (2, 4), (7, 8)), ((0, 0), (0, 0), (6, 8), (0, 0)),),
)
MESH = pl.DeviceIdType.MESH


def exchange_kernel(
    n, peers, groups, cap, width, hidden, tasks,
    counts_hbm, gate_hbm, ids_hbm, x_hbm, cot_hbm, w1_hbm, w2_hbm,
    first, second, home,
    counts_ref, gate_ref, ids_ref, cots, tag, pay, buf, w1, w2, w1_turned, w2_turned, ret, act, pc,
    send1, recv1, send2, recv2, send3, recv3, local_sem, ready, turn_sem,
):
    b = lax.axis_index("blk")
    h = lax.axis_index("dp")
    half, quarter = n // 2, n // 4
    early = n - quarter
    width_part = width // peers
    hidden_part = hidden // peers
    tiles = hidden // tile
    part_tiles = hidden_part // tile
    side, place = b // half, lax.rem(b, half)
    step, spot = place // quarter, lax.rem(place, quarter)

    z = 2 * side + step

    def device_at(floor, shift):
        return floor * quarter + lax.rem(spot + shift, quarter)

    def near_target(i):
        return device_at(2 * side + step, quarter - i)

    def cross_target(i):
        return device_at(2 * side + 1 - step, quarter - i)

    def far_target(i):
        return device_at(2 - 2 * side + lax.rem(i, 2), quarter - i // 2)

    def far_slot(i):
        return (1 + 2 * lax.rem(side + step, 2)) * quarter + i // 2

    def near_source(i):
        return device_at(2 * side + step, i)

    def outer_source(i):
        return device_at(3 - 3 * side, i)

    def cross_source(i):
        return device_at(2 * side + 1 - step, i)

    def inner_source(i):
        return device_at(2 - side, i)

    def slot_rows(i):
        return pl.ds(pl.multiple_of(i * cap, cap), cap)

    span = half * cap

    def buf_rows(j, i):
        return pl.ds(pl.multiple_of((i // half * peers + j) * span + lax.rem(i, half) * cap, cap), cap)

    barrier = pltpu.get_barrier_semaphore()

    def greet(target, j):
        pl.semaphore_signal(barrier, inc=1, device_id=(target, lax.rem(h + j, peers)), device_id_type=MESH)

    @pl.when(side == 0)
    def _():
        @pl.loop(1, n)
        def _(k):
            greet(lax.rem(b + k, n), 0)

        for j in range(1, peers):
            @pl.loop(0, quarter)
            def _(i):
                greet(near_target(i), j)

    @pl.when(z == 2)
    def _():
        for j in range(peers):
            @pl.loop(0, quarter)
            def _(i):
                greet(cross_target(i), j)

    loads = [
        pltpu.make_async_copy(source, target, local_sem.at[6 + at])
        for at, (source, target) in enumerate(
            [(x_hbm, pay.at[pl.ds(r * groups, groups), :, pl.ds(0, width)]) for r in range(n // groups)]
            + [(counts_hbm, counts_ref), (gate_hbm, gate_ref), (ids_hbm, ids_ref), (cot_hbm, cots)]
        )
    ]
    for load in loads[:-4]:
        load.start()

    def call(k, target, j):
        pl.semaphore_signal(ready.at[k], inc=1, device_id=(target, lax.rem(h + j, peers)), device_id_type=MESH)

    @pl.when(z == 2)
    def _():
        pl.semaphore_wait(barrier, half)

        @pl.loop(0, half)
        def _(i):
            call(0, half - 1 - i, 0)

    @pl.when(z == 3)
    def _():
        pl.semaphore_wait(barrier, half + quarter * peers)

        @pl.loop(0, half)
        def _(i):
            call(1, i, 0)

        for j in range(peers):
            @pl.loop(0, quarter)
            def _(i):
                call(1, cross_target(i), j)

    for load in loads[-4:]:
        load.start()
    get_w1 = pltpu.make_async_copy(w1_hbm.at[0], w1, local_sem.at[3])

    def get_w2(q):
        return pltpu.make_async_copy(w2_hbm.at[0, pl.ds(q * tile, tile)], w2.at[q % 2], turn_sem.at[q])

    get_w1.start()
    for q in range(2):
        get_w2(q).start()

    ahead = quarter // 2

    def far_part(i, part):
        target = far_target(i)
        columns = pl.ds(part * width, width)
        return pltpu.make_async_remote_copy(
            src_ref=pay.at[target, :, columns], dst_ref=buf.at[buf_rows(0, far_slot(i)), columns],
            send_sem=send1.at[0], recv_sem=recv1.at[far_slot(i)],
            device_id=(target, h), device_id_type=MESH,
        )

    for load in loads[:-4]:
        load.wait()

    @pl.when(z == 2)
    def _():
        @pl.loop(0, ahead)
        def _(i):
            far_part(i, 0).start()

    for load in loads[-4:]:
        load.wait()
    slots = groups * cap
    lanes = lax.broadcasted_iota(jnp.int32, (slots, slots), 1)
    places = lax.broadcasted_iota(jnp.int32, (slots, slots), 0)
    ids = jnp.broadcast_to(ids_ref[...].astype(jnp.float32), (slots, slots))
    tag[...] = jnp.broadcast_to(
        jnp.sum(jnp.where(lanes == places, ids, 0.0), axis=1, keepdims=True), tag.shape
    )
    order = lax.broadcasted_iota(jnp.int32, (cap, 1), 0)

    @pl.loop(0, groups)
    def _(g):
        known = tag[slot_rows(g), :][:, 0:1]
        live = order < counts_ref[0, g]
        cot_rows = cots[g].astype(jnp.float32)
        for r in range(n // groups):
            gate = jnp.zeros((cap, 1), jnp.float32)
            for t in range(tasks):
                gate = jnp.where(known == float(t), gate_ref[t, r * groups + g], gate)
            gate = jnp.where(live, gate, 0.0)
            pay[r * groups + g, :, pl.ds(width, width)] = (gate * cot_rows).astype(jnp.bfloat16)

    own = pltpu.make_async_copy(pay.at[b], buf.at[pl.ds(0, cap)], local_sem.at[2])
    own.start()

    def block_out(target, slot):
        return pltpu.make_async_remote_copy(
            src_ref=pay.at[target], dst_ref=buf.at[buf_rows(0, slot)],
            send_sem=send1.at[0], recv_sem=recv1.at[slot],
            device_id=(target, h), device_id_type=MESH,
        )

    def forward(i, j):
        return pltpu.make_async_remote_copy(
            src_ref=buf.at[buf_rows(0, i)], dst_ref=buf.at[buf_rows(j, i)],
            send_sem=send2.at[j - 1], recv_sem=recv2.at[j - 1, i // half],
            device_id=(b, lax.rem(h + j, peers)), device_id_type=MESH,
        )

    def across(i, j):
        target = near_target(i)
        return pltpu.make_async_remote_copy(
            src_ref=pay.at[target], dst_ref=buf.at[buf_rows(j, i)],
            send_sem=send2.at[j - 1], recv_sem=recv2.at[j - 1, i // half],
            device_id=(target, lax.rem(h + j, peers)), device_id_type=MESH,
        )

    def homeward(i, target):
        return pltpu.make_async_remote_copy(
            src_ref=ret.at[slot_rows(i)], dst_ref=home.at[b],
            send_sem=send3.at[0], recv_sem=recv3.at[0],
            device_id=(target, h), device_id_type=MESH,
        )

    def pass_on(i):
        block_out(b, i).wait_recv()
        for j in range(1, peers):
            forward(i, j).start()

    def send_far(start, stop, stride):
        @pl.loop(start, stop, step=stride)
        def _(i):
            block_out(far_target(i), far_slot(i)).start()

    def send_near():
        for j in range(1, peers):
            @pl.loop(0, quarter)
            def _(i):
                across(i, j).start()

        @pl.loop(1, quarter)
        def _(i):
            block_out(near_target(i), i).start()

    def send_cross():
        @pl.loop(0, quarter)
        def _(i):
            block_out(cross_target(i), half + i).start()

    @pl.when(side == 0)
    def _():
        pl.semaphore_wait(barrier, half - 1 + (peers - 1) * quarter)
        send_near()

        @pl.when(step == 1)
        def _():
            send_cross()

        pl.semaphore_wait(ready.at[0], quarter)
        send_far(0, quarter, 2)
        pl.semaphore_wait(ready.at[1], quarter)
        send_far(1, quarter, 2)
        send_far(quarter, half, 1)

        @pl.when(step == 0)
        def _():
            send_cross()

    @pl.when(z == 2)
    def _():
        @pl.loop(0, ahead)
        def _(i):
            far_part(i, 1).start()

        send_far(ahead, half, 1)
        pl.semaphore_wait(ready.at[1], quarter * peers)
        call(0, cross_target(0), 0)
        send_near()
        send_cross()

    @pl.when(z == 3)
    def _():
        send_far(0, half, 1)
        send_cross()
        pl.semaphore_wait(ready.at[0], 1)
        send_near()

    schedule = iter(SCHEDULE)

    def pick(values):
        value = values[0]
        for floor in range(1, 4):
            value = jnp.where(z == floor, values[floor], value)
        return value * quarter // 4

    def poll(wanted=True):
        if not wanted:
            return
        for ranges in next(schedule):
            @pl.loop(half + pick([start for start, _ in ranges]), half + pick([stop for _, stop in ranges]))
            def _(i):
                pass_on(i)

    get_w1.wait()
    for q in range(tiles):
        part = pl.ds(q * tile, tile)
        get_w2(q).wait()
        w2_turned[:, part] = w2[q % 2].T
        if q + 2 < tiles:
            get_w2(q + 2).start()
        w1_turned[part, :] = w1[:, part].T

    @pl.loop(quarter, half)
    def _(i):
        pass_on(i)

    poll()

    @pl.loop(1, quarter)
    def _(i):
        block_out(b, i).wait_recv()

    own.wait()

    def rows_forward(start, total, hook=lambda q: None):
        rows = pl.ds(start, total)

        def hidden_tile(q):
            at = lax.rem(h * hidden_part + q * tile, hidden)
            columns = pl.ds(pl.multiple_of(at, tile), tile)
            pre = jnp.dot(
                buf[rows, pl.ds(0, width)], w1[:, columns], preferred_element_type=jnp.float32
            )
            sig = jax.nn.sigmoid(pre)
            if q < part_tiles:
                act[rows, pl.ds(q * tile, tile)] = (pre * sig).astype(jnp.bfloat16)
            cot = jnp.dot(
                buf[rows, pl.ds(width, width)], w2_turned[:, columns], preferred_element_type=jnp.float32
            )
            pc[rows, columns] = (cot * (sig * (1.0 + pre * (1.0 - sig)))).astype(jnp.bfloat16)

        for q in range(tiles):
            hidden_tile(q)
            hook(q)

    def rows_home(part, hook=lambda d: None):
        rows = pl.ds(part * span, span)
        flat = pl.ds(part * peers * span, span)

        for d in range(width // tile):
            columns = pl.ds(d * tile, tile)
            grad = jnp.dot(pc[flat, :], w1_turned[:, columns], preferred_element_type=jnp.float32)
            ret[rows, columns] = grad.astype(jnp.bfloat16)
            hook(d)

    def partner_come(part):
        for j in range(1, peers):
            rows = buf.at[pl.ds((part * peers + j) * span, span)]
            pltpu.make_async_copy(rows, rows, recv2.at[j - 1, part]).wait()

    turned = (((0,), (0,)), ((), ()))
    chunk = peers * span

    def grads(part, hook=lambda: None):
        rows = pl.ds(part * chunk, chunk)

        def add(out, columns, left, right):
            grad = lax.dot_general(left, right, turned, preferred_element_type=jnp.float32)
            if part:
                grad = (out[:, columns] + grad) * grad_scale
            out[:, columns] = grad

        for q in range(tiles):
            columns = pl.ds(q * tile, tile)
            add(first, columns, buf[rows, pl.ds(pl.multiple_of(h * width_part, width_part), width_part)], pc[rows, columns])
        hook()
        for q in range(width // tile):
            columns = pl.ds(q * tile, tile)
            add(second, columns, act[rows, :], buf[rows, pl.ds(width + q * tile, tile)])

    def release(point):
        @pl.when(pick([4 * (point == chosen) for chosen in RELEASE]) > 0)
        def _():
            @pl.loop(quarter, half)
            def _(i):
                homeward(i, outer_source(i)).start()

    def between():
        poll()
        release(1)

    rows_forward(0, span)
    poll()
    rows_home(0, lambda d: poll(d == 0))
    own_home = pltpu.make_async_copy(ret.at[pl.ds(0, cap)], home.at[b], local_sem.at[5])
    own_home.start()

    @pl.loop(1, quarter)
    def _(i):
        homeward(i, near_source(i)).start()

    poll()
    partner_come(0)
    rows_forward(span, chunk - span, lambda q: poll(2 * (q + 1) == tiles))
    poll()
    release(0)
    grads(0, between)
    poll()

    release(2)

    rows_forward(chunk, span)
    rows_home(1)

    @pl.loop(early, n)
    def _(i):
        homeward(i, inner_source(i)).start()

    @pl.loop(half, early)
    def _(i):
        homeward(i, cross_source(i)).start()

    partner_come(1)
    rows_forward(chunk + span, chunk - span)

    grads(1)

    own_home.wait()

    sent = pay.at[pl.ds(0, n - 1)]
    pltpu.make_async_copy(sent, sent, send1.at[0]).wait()
    for j in range(1, peers):
        whole = buf.at[pl.ds(0, 2 * span)]
        pltpu.make_async_copy(whole, whole, send2.at[j - 1]).wait()
    gone = ret.at[pl.ds(0, (n - 1) * cap)]
    pltpu.make_async_copy(gone, gone, send3.at[0]).wait()

    come = home.at[pl.ds(0, n - 1)]
    pltpu.make_async_copy(come, come, recv3.at[0]).wait()


def finish_kernel(first, second, home, out_rows, out_first, out_second, rows, sem):
    puts = []
    for source, target in ((first, out_first), (second, out_second)):
        step = source.shape[0] // PIECES
        for piece in range(PIECES):
            part = pl.ds(piece * step, step)
            puts.append(pltpu.make_async_copy(source.at[part], target.at[0, part], sem.at[len(puts)]))
            puts[-1].start()
    repeats, total = home.shape[0], jnp.float32(0.0)
    for r in range(repeats):
        total = total + home[r].astype(jnp.float32)
    rows[...] = total
    puts.append(pltpu.make_async_copy(rows, out_rows, sem.at[len(puts)]))
    puts[-1].start()
    for put in puts:
        put.wait()


def on_device(n, peers, inputs, cotangent, task_ids, group_counts, task_gate, w_in, w_out):
    groups = group_counts.shape[1]
    slots, width = inputs.shape
    hidden = w_in.shape[2]
    cap = slots // groups
    tasks = task_gate.shape[0]
    rows = peers * n * cap
    bf16 = jnp.bfloat16
    hbm = pl.BlockSpec(memory_space=pltpu.HBM)
    vmem = pl.BlockSpec(memory_space=pltpu.VMEM)
    dma = pltpu.SemaphoreType.DMA
    first, second, home = pl.pallas_call(
        functools.partial(exchange_kernel, n, peers, groups, cap, width, hidden, tasks),
        out_shape=(
            pltpu.VMEM((width // peers, hidden), jnp.float32),
            pltpu.VMEM((hidden // peers, width), jnp.float32),
            pltpu.VMEM((n, cap, width), bf16),
        ),
        in_specs=[hbm] * 7,
        out_specs=(vmem,) * 3,
        scratch_shapes=[
            pltpu.SMEM(group_counts.shape, jnp.int32),
            pltpu.SMEM(task_gate.shape, jnp.float32),
            pltpu.VMEM((1, slots), jnp.int32),
            pltpu.VMEM((groups, cap, width), bf16),
            pltpu.VMEM((slots, slots), jnp.float32),
            pltpu.VMEM((n, cap, 2 * width), bf16),
            pltpu.VMEM((rows, 2 * width), bf16),
            pltpu.VMEM((width, hidden), bf16),
            pltpu.VMEM((2, tile, width), bf16),
            pltpu.VMEM((hidden, width), bf16),
            pltpu.VMEM((width, hidden), bf16),
            pltpu.VMEM((n * cap, width), bf16),
            pltpu.VMEM((rows, hidden // peers), bf16),
            pltpu.VMEM((rows, hidden), bf16),
            dma((1,)), dma((n,)), dma((peers - 1,)), dma((peers - 1, 2)), dma((1,)), dma((1,)),
            dma((10 + n // groups,)),
            pltpu.SemaphoreType.REGULAR((2,)),
            dma((hidden // tile,)),
        ],
        compiler_params=pltpu.CompilerParams(
            collective_id=0, has_side_effects=True, vmem_limit_bytes=VMEM_BYTES
        ),
    )(
        *(
            pltpu.with_memory_space_constraint(array, pltpu.HBM)
            for array in (
                group_counts, task_gate, task_ids.reshape(1, slots), inputs.reshape(groups, cap, width),
                cotangent.reshape(groups, cap, width), w_in, w_out,
            )
        )
    )
    return pl.pallas_call(
        finish_kernel,
        out_shape=(
            jax.ShapeDtypeStruct((slots, width), jnp.float32),
            jax.ShapeDtypeStruct((1,) + first.shape, jnp.float32),
            jax.ShapeDtypeStruct((1,) + second.shape, jnp.float32),
        ),
        in_specs=[vmem] * 3,
        out_specs=(hbm,) * 3,
        scratch_shapes=[pltpu.VMEM((slots, width), jnp.float32), dma((2 * PIECES + 1,))],
        compiler_params=pltpu.CompilerParams(vmem_limit_bytes=4 * 1024 * 1024),
    )(first, second, home.reshape(n // groups, slots, width))


def solution(mesh):
    in_specs = (
        P(("blk", "dp"), None),
        P(("blk", "dp"), None),
        P(("blk", "dp")),
        P(("blk", "dp"), None),
        P(),
        P("blk", None, None),
        P("blk", None, None),
    )
    out_specs = (P(("blk", "dp"), None), P("blk", "dp", None), P("blk", "dp", None))
    body = functools.partial(on_device, mesh.shape["blk"], mesh.shape["dp"])
    return jax.shard_map(body, mesh=mesh, in_specs=in_specs, out_specs=out_specs, check_vma=False)
```

```python
import functools

import jax
import jax.numpy as jnp
from jax import lax
from jax.experimental import pallas as pl
from jax.experimental.pallas import tpu as pltpu
from jax.sharding import PartitionSpec as P

grad_scale = 0.0625
VMEM_BYTES = 51 * 1024 * 1024
PIECES = 4
RELEASE = (2, 9, 9, 1)
tile = 512
SCHEDULE = (
    (((0, 4), (0, 0), (0, 0), (0, 4)),),
    (((0, 0), (0, 1), (0, 0), (0, 0)),),
    (((0, 0), (1, 2), (0, 0), (0, 0)),),
    (((4, 6), (0, 0), (4, 6), (4, 5)),),
    (((0, 0), (2, 3), (0, 0), (0, 0)),),
    (((0, 0), (3, 6), (0, 2), (5, 6)),),
    (((6, 7), (6, 7), (0, 0), (6, 7)),),
    (((7, 8), (7, 8), (2, 4), (7, 8)), ((0, 0), (0, 0), (6, 8), (0, 0)),),
)
MESH = pl.DeviceIdType.MESH


def exchange_kernel(
    n, peers, groups, cap, width, hidden, tasks,
    counts_hbm, gate_hbm, ids_hbm, x_hbm, cot_hbm, w1_hbm, w2_hbm,
    first, second, home,
    counts_ref, gate_ref, ids_ref, cots, tag, pay, buf, w1, w2, w1_turned, w2_turned, ret, act, pc,
    send1, recv1, send2, recv2, send3, recv3, local_sem, ready, turn_sem,
):
    b = lax.axis_index("blk")
    h = lax.axis_index("dp")
    half, quarter = n // 2, n // 4
    early = n - quarter
    width_part = width // peers
    hidden_part = hidden // peers
    tiles = hidden // tile
    part_tiles = hidden_part // tile
    side, place = b // half, lax.rem(b, half)
    step, spot = place // quarter, lax.rem(place, quarter)

    z = 2 * side + step

    def device_at(floor, shift):
        return floor * quarter + lax.rem(spot + shift, quarter)

    def near_target(i):
        return device_at(2 * side + step, quarter - i)

    def cross_target(i):
        return device_at(2 * side + 1 - step, quarter - i)

    def far_target(i):
        return device_at(2 - 2 * side + lax.rem(i, 2), quarter - i // 2)

    def far_slot(i):
        return (1 + 2 * lax.rem(side + step, 2)) * quarter + i // 2

    def near_source(i):
        return device_at(2 * side + step, i)

    def outer_source(i):
        return device_at(3 - 3 * side, i)

    def cross_source(i):
        return device_at(2 * side + 1 - step, i)

    def inner_source(i):
        return device_at(2 - side, i)

    def slot_rows(i):
        return pl.ds(pl.multiple_of(i * cap, cap), cap)

    span = half * cap

    def buf_rows(j, i):
        return pl.ds(pl.multiple_of((i // half * peers + j) * span + lax.rem(i, half) * cap, cap), cap)

    barrier = pltpu.get_barrier_semaphore()

    def greet(target, j):
        pl.semaphore_signal(barrier, inc=1, device_id=(target, lax.rem(h + j, peers)), device_id_type=MESH)

    @pl.when(side == 0)
    def _():
        @pl.loop(1, n)
        def _(k):
            greet(lax.rem(b + k, n), 0)

        for j in range(1, peers):
            @pl.loop(0, quarter)
            def _(i):
                greet(near_target(i), j)

    @pl.when(z == 2)
    def _():
        for j in range(peers):
            @pl.loop(0, quarter)
            def _(i):
                greet(cross_target(i), j)

    loads = [
        pltpu.make_async_copy(source, target, local_sem.at[6 + at])
        for at, (source, target) in enumerate(
            [(x_hbm, pay.at[pl.ds(r * groups, groups), :, pl.ds(0, width)]) for r in range(n // groups)]
            + [(counts_hbm, counts_ref), (gate_hbm, gate_ref), (ids_hbm, ids_ref), (cot_hbm, cots)]
        )
    ]
    for load in loads:
        load.start()

    def call(k, target, j):
        pl.semaphore_signal(ready.at[k], inc=1, device_id=(target, lax.rem(h + j, peers)), device_id_type=MESH)

    @pl.when(z == 2)
    def _():
        pl.semaphore_wait(barrier, half)

        @pl.loop(0, half)
        def _(i):
            call(0, half - 1 - i, 0)

    @pl.when(z == 3)
    def _():
        pl.semaphore_wait(barrier, half + quarter * peers)

        @pl.loop(0, half)
        def _(i):
            call(1, i, 0)

        for j in range(peers):
            @pl.loop(0, quarter)
            def _(i):
                call(1, cross_target(i), j)

    get_w1 = pltpu.make_async_copy(w1_hbm.at[0], w1, local_sem.at[3])

    def get_w2(q):
        return pltpu.make_async_copy(w2_hbm.at[0, pl.ds(q * tile, tile)], w2.at[q % 2], turn_sem.at[q])

    get_w1.start()
    for q in range(2):
        get_w2(q).start()

    ahead = quarter // 2

    def far_part(i, part):
        target = far_target(i)
        columns = pl.ds(part * width, width)
        return pltpu.make_async_remote_copy(
            src_ref=pay.at[target, :, columns], dst_ref=buf.at[buf_rows(0, far_slot(i)), columns],
            send_sem=send1.at[1], recv_sem=recv1.at[far_slot(i)],
            device_id=(target, h), device_id_type=MESH,
        )

    for load in loads[:-4]:
        load.wait()

    @pl.when(z == 2)
    def _():
        @pl.loop(0, ahead)
        def _(i):
            far_part(i, 0).start()

    for load in loads[-4:]:
        load.wait()
    slots = groups * cap
    lanes = lax.broadcasted_iota(jnp.int32, (slots, slots), 1)
    places = lax.broadcasted_iota(jnp.int32, (slots, slots), 0)
    ids = jnp.broadcast_to(ids_ref[...].astype(jnp.float32), (slots, slots))
    tag[...] = jnp.broadcast_to(
        jnp.sum(jnp.where(lanes == places, ids, 0.0), axis=1, keepdims=True), tag.shape
    )
    order = lax.broadcasted_iota(jnp.int32, (cap, 1), 0)

    @pl.loop(0, groups)
    def _(g):
        known = tag[slot_rows(g), :][:, 0:1]
        live = order < counts_ref[0, g]
        cot_rows = cots[g].astype(jnp.float32)
        for r in range(n // groups):
            gate = jnp.zeros((cap, 1), jnp.float32)
            for t in range(tasks):
                gate = jnp.where(known == float(t), gate_ref[t, r * groups + g], gate)
            gate = jnp.where(live, gate, 0.0)
            pay[r * groups + g, :, pl.ds(width, width)] = (gate * cot_rows).astype(jnp.bfloat16)

    own = pltpu.make_async_copy(pay.at[b], buf.at[pl.ds(0, cap)], local_sem.at[2])
    own.start()

    def block_out(target, slot, kind=0):
        return pltpu.make_async_remote_copy(
            src_ref=pay.at[target], dst_ref=buf.at[buf_rows(0, slot)],
            send_sem=send1.at[kind], recv_sem=recv1.at[slot],
            device_id=(target, h), device_id_type=MESH,
        )

    def forward(i, j):
        return pltpu.make_async_remote_copy(
            src_ref=buf.at[buf_rows(0, i)], dst_ref=buf.at[buf_rows(j, i)],
            send_sem=send2.at[j - 1], recv_sem=recv2.at[j - 1, i // half],
            device_id=(b, lax.rem(h + j, peers)), device_id_type=MESH,
        )

    def across(i, j):
        target = near_target(i)
        return pltpu.make_async_remote_copy(
            src_ref=pay.at[target], dst_ref=buf.at[buf_rows(j, i)],
            send_sem=send2.at[j - 1], recv_sem=recv2.at[j - 1, i // half],
            device_id=(target, lax.rem(h + j, peers)), device_id_type=MESH,
        )

    def homeward(i, target):
        return pltpu.make_async_remote_copy(
            src_ref=ret.at[slot_rows(i)], dst_ref=home.at[b],
            send_sem=send3.at[0], recv_sem=recv3.at[0],
            device_id=(target, h), device_id_type=MESH,
        )

    def pass_on(i):
        block_out(b, i).wait_recv()
        for j in range(1, peers):
            forward(i, j).start()

    def send_far(start, stop, stride):
        @pl.loop(start, stop, step=stride)
        def _(i):
            block_out(far_target(i), far_slot(i), 1).start()

    def send_near():
        for j in range(1, peers):
            @pl.loop(0, quarter)
            def _(i):
                across(i, j).start()

        @pl.loop(1, quarter)
        def _(i):
            block_out(near_target(i), i).start()

    def send_cross():
        @pl.loop(0, quarter)
        def _(i):
            block_out(cross_target(i), half + i).start()

    @pl.when(side == 0)
    def _():
        pl.semaphore_wait(barrier, half - 1 + (peers - 1) * quarter)
        send_near()

        @pl.when(step == 1)
        def _():
            send_cross()

        pl.semaphore_wait(ready.at[0], quarter)
        send_far(0, quarter, 2)
        pl.semaphore_wait(ready.at[1], quarter)
        send_far(1, quarter, 2)
        send_far(quarter, half, 1)

        @pl.when(step == 0)
        def _():
            send_cross()

    @pl.when(z == 2)
    def _():
        @pl.loop(0, ahead)
        def _(i):
            far_part(i, 1).start()

        send_far(ahead, half, 1)
        pl.semaphore_wait(ready.at[1], quarter * peers)
        call(0, cross_target(0), 0)
        send_near()
        send_cross()

    @pl.when(z == 3)
    def _():
        send_far(0, half, 1)
        send_cross()
        pl.semaphore_wait(ready.at[0], 1)
        send_near()

    schedule = iter(SCHEDULE)

    def pick(values):
        value = values[0]
        for floor in range(1, 4):
            value = jnp.where(z == floor, values[floor], value)
        return value * quarter // 4

    def poll(wanted=True):
        if not wanted:
            return
        for ranges in next(schedule):
            @pl.loop(half + pick([start for start, _ in ranges]), half + pick([stop for _, stop in ranges]))
            def _(i):
                pass_on(i)

    get_w1.wait()
    for q in range(tiles):
        part = pl.ds(q * tile, tile)
        get_w2(q).wait()
        w2_turned[:, part] = w2[q % 2].T
        if q + 2 < tiles:
            get_w2(q + 2).start()
        w1_turned[part, :] = w1[:, part].T

    @pl.loop(quarter, half)
    def _(i):
        pass_on(i)

    poll()

    @pl.loop(1, quarter)
    def _(i):
        block_out(b, i).wait_recv()

    own.wait()

    def rows_forward(start, total, hook=lambda q: None):
        rows = pl.ds(start, total)

        def hidden_tile(q):
            at = lax.rem(h * hidden_part + q * tile, hidden)
            columns = pl.ds(pl.multiple_of(at, tile), tile)
            pre = jnp.dot(
                buf[rows, pl.ds(0, width)], w1[:, columns], preferred_element_type=jnp.float32
            )
            sig = jax.nn.sigmoid(pre)
            if q < part_tiles:
                act[rows, pl.ds(q * tile, tile)] = (pre * sig).astype(jnp.bfloat16)
            cot = jnp.dot(
                buf[rows, pl.ds(width, width)], w2_turned[:, columns], preferred_element_type=jnp.float32
            )
            pc[rows, columns] = (cot * (sig * (1.0 + pre * (1.0 - sig)))).astype(jnp.bfloat16)

        for q in range(tiles):
            hidden_tile(q)
            hook(q)

    def rows_home(part, hook=lambda d: None):
        rows = pl.ds(part * span, span)
        flat = pl.ds(part * peers * span, span)

        for d in range(width // tile):
            columns = pl.ds(d * tile, tile)
            grad = jnp.dot(pc[flat, :], w1_turned[:, columns], preferred_element_type=jnp.float32)
            ret[rows, columns] = grad.astype(jnp.bfloat16)
            hook(d)

    def partner_come(part):
        for j in range(1, peers):
            rows = buf.at[pl.ds((part * peers + j) * span, span)]
            pltpu.make_async_copy(rows, rows, recv2.at[j - 1, part]).wait()

    turned = (((0,), (0,)), ((), ()))
    chunk = peers * span

    def grads(part, hook=lambda: None):
        rows = pl.ds(part * chunk, chunk)

        def add(out, columns, left, right):
            grad = lax.dot_general(left, right, turned, preferred_element_type=jnp.float32)
            if part:
                grad = (out[:, columns] + grad) * grad_scale
            out[:, columns] = grad

        for q in range(tiles):
            columns = pl.ds(q * tile, tile)
            add(first, columns, buf[rows, pl.ds(pl.multiple_of(h * width_part, width_part), width_part)], pc[rows, columns])
        hook()
        for q in range(width // tile):
            columns = pl.ds(q * tile, tile)
            add(second, columns, act[rows, :], buf[rows, pl.ds(width + q * tile, tile)])

    outer = lax.rem(side + step, 2) == 0

    def far_sent():
        sent = pay.at[pl.ds(0, half)]
        pltpu.make_async_copy(sent, sent, send1.at[1]).wait()

    kept = half - (1 - side) * (quarter // 4)

    def send_outer(start, stop):
        @pl.loop(start, stop)
        def _(i):
            homeward(i, outer_source(i)).start()

    def release(point):
        @pl.when(pick([4 * (point == chosen) for chosen in RELEASE]) > 0)
        def _():
            send_outer(quarter, kept)

    def between():
        poll()
        release(1)

    rows_forward(0, span)
    poll()
    rows_home(0, lambda d: poll(d == 0))
    own_home = pltpu.make_async_copy(ret.at[pl.ds(0, cap)], home.at[b], local_sem.at[5])
    own_home.start()

    @pl.loop(1, quarter)
    def _(i):
        homeward(i, near_source(i)).start()

    poll()
    partner_come(0)
    rows_forward(span, chunk - span, lambda q: poll(2 * (q + 1) == tiles))
    poll()
    release(0)
    grads(0, between)

    @pl.when(jnp.logical_not(outer))
    def _():
        far_sent()
        send_outer(quarter, kept)

    poll()

    release(2)

    rows_forward(chunk, span)
    rows_home(1)

    @pl.loop(early, n)
    def _(i):
        homeward(i, inner_source(i)).start()

    send_outer(kept, half)

    @pl.loop(half, early)
    def _(i):
        homeward(i, cross_source(i)).start()

    partner_come(1)
    rows_forward(chunk + span, chunk - span)

    grads(1)

    own_home.wait()

    sent = pay.at[pl.ds(0, half - 1)]
    pltpu.make_async_copy(sent, sent, send1.at[0]).wait()

    @pl.when(outer)
    def _():
        far_sent()

    for j in range(1, peers):
        whole = buf.at[pl.ds(0, 2 * span)]
        pltpu.make_async_copy(whole, whole, send2.at[j - 1]).wait()
    gone = ret.at[pl.ds(0, (n - 1) * cap)]
    pltpu.make_async_copy(gone, gone, send3.at[0]).wait()

    come = home.at[pl.ds(0, n - 1)]
    pltpu.make_async_copy(come, come, recv3.at[0]).wait()


def finish_kernel(first, second, home, out_rows, out_first, out_second, rows, sem):
    puts = []
    for source, target in ((first, out_first), (second, out_second)):
        step = source.shape[0] // PIECES
        for piece in range(PIECES):
            part = pl.ds(piece * step, step)
            puts.append(pltpu.make_async_copy(source.at[part], target.at[0, part], sem.at[len(puts)]))
            puts[-1].start()
    repeats, total = home.shape[0], jnp.float32(0.0)
    for r in range(repeats):
        total = total + home[r].astype(jnp.float32)
    rows[...] = total
    puts.append(pltpu.make_async_copy(rows, out_rows, sem.at[len(puts)]))
    puts[-1].start()
    for put in puts:
        put.wait()


def on_device(n, peers, inputs, cotangent, task_ids, group_counts, task_gate, w_in, w_out):
    groups = group_counts.shape[1]
    slots, width = inputs.shape
    hidden = w_in.shape[2]
    cap = slots // groups
    tasks = task_gate.shape[0]
    rows = peers * n * cap
    bf16 = jnp.bfloat16
    hbm = pl.BlockSpec(memory_space=pltpu.HBM)
    vmem = pl.BlockSpec(memory_space=pltpu.VMEM)
    dma = pltpu.SemaphoreType.DMA
    first, second, home = pl.pallas_call(
        functools.partial(exchange_kernel, n, peers, groups, cap, width, hidden, tasks),
        out_shape=(
            pltpu.VMEM((width // peers, hidden), jnp.float32),
            pltpu.VMEM((hidden // peers, width), jnp.float32),
            pltpu.VMEM((n, cap, width), bf16),
        ),
        in_specs=[hbm] * 7,
        out_specs=(vmem,) * 3,
        scratch_shapes=[
            pltpu.SMEM(group_counts.shape, jnp.int32),
            pltpu.SMEM(task_gate.shape, jnp.float32),
            pltpu.VMEM((1, slots), jnp.int32),
            pltpu.VMEM((groups, cap, width), bf16),
            pltpu.VMEM((slots, slots), jnp.float32),
            pltpu.VMEM((n, cap, 2 * width), bf16),
            pltpu.VMEM((rows, 2 * width), bf16),
            pltpu.VMEM((width, hidden), bf16),
            pltpu.VMEM((2, tile, width), bf16),
            pltpu.VMEM((hidden, width), bf16),
            pltpu.VMEM((width, hidden), bf16),
            pltpu.VMEM((n * cap, width), bf16),
            pltpu.VMEM((rows, hidden // peers), bf16),
            pltpu.VMEM((rows, hidden), bf16),
            dma((2,)), dma((n,)), dma((peers - 1,)), dma((peers - 1, 2)), dma((1,)), dma((1,)),
            dma((10 + n // groups,)),
            pltpu.SemaphoreType.REGULAR((2,)),
            dma((hidden // tile,)),
        ],
        compiler_params=pltpu.CompilerParams(
            collective_id=0, has_side_effects=True, vmem_limit_bytes=VMEM_BYTES
        ),
    )(
        *(
            pltpu.with_memory_space_constraint(array, pltpu.HBM)
            for array in (
                group_counts, task_gate, task_ids.reshape(1, slots), inputs.reshape(groups, cap, width),
                cotangent.reshape(groups, cap, width), w_in, w_out,
            )
        )
    )
    return pl.pallas_call(
        finish_kernel,
        out_shape=(
            jax.ShapeDtypeStruct((slots, width), jnp.float32),
            jax.ShapeDtypeStruct((1,) + first.shape, jnp.float32),
            jax.ShapeDtypeStruct((1,) + second.shape, jnp.float32),
        ),
        in_specs=[vmem] * 3,
        out_specs=(hbm,) * 3,
        scratch_shapes=[pltpu.VMEM((slots, width), jnp.float32), dma((2 * PIECES + 1,))],
        compiler_params=pltpu.CompilerParams(vmem_limit_bytes=4 * 1024 * 1024),
    )(first, second, home.reshape(n // groups, slots, width))


def solution(mesh):
    in_specs = (
        P(("blk", "dp"), None),
        P(("blk", "dp"), None),
        P(("blk", "dp")),
        P(("blk", "dp"), None),
        P(),
        P("blk", None, None),
        P("blk", None, None),
    )
    out_specs = (P(("blk", "dp"), None), P("blk", "dp", None), P("blk", "dp", None))
    body = functools.partial(on_device, mesh.shape["blk"], mesh.shape["dp"])
    return jax.shard_map(body, mesh=mesh, in_specs=in_specs, out_specs=out_specs, check_vma=False)
```

```python
import functools

import jax
import jax.numpy as jnp
from jax import lax
from jax.experimental import pallas as pl
from jax.experimental.pallas import tpu as pltpu
from jax.sharding import PartitionSpec as P

grad_scale = 0.0625
VMEM_BYTES = 51 * 1024 * 1024
PIECES = 4
RELEASE = (2, 9, 9, 1)
tile = 512
SCHEDULE = (
    (((0, 4), (0, 0), (0, 0), (0, 4)),),
    (((0, 0), (0, 1), (0, 0), (0, 0)),),
    (((0, 0), (1, 2), (0, 0), (0, 0)),),
    (((4, 6), (0, 0), (4, 6), (4, 5)),),
    (((0, 0), (2, 3), (0, 0), (0, 0)),),
    (((0, 0), (3, 6), (0, 2), (5, 6)),),
    (((6, 7), (6, 7), (0, 0), (6, 7)),),
    (((7, 8), (7, 8), (2, 4), (7, 8)), ((0, 0), (0, 0), (6, 8), (0, 0)),),
)
MESH = pl.DeviceIdType.MESH


def exchange_kernel(
    n, peers, groups, cap, width, hidden, tasks,
    counts_hbm, gate_hbm, ids_hbm, x_hbm, cot_hbm, w1_hbm, w2_hbm,
    first, second, home,
    counts_ref, gate_ref, ids_ref, cots, tag, pay, buf, w1, w2, w1_turned, w2_turned, ret, act, pc,
    send1, recv1, send2, recv2, send3, recv3, local_sem, ready, turn_sem,
):
    b = lax.axis_index("blk")
    h = lax.axis_index("dp")
    half, quarter = n // 2, n // 4
    early = n - quarter
    width_part = width // peers
    hidden_part = hidden // peers
    tiles = hidden // tile
    part_tiles = hidden_part // tile
    side, place = b // half, lax.rem(b, half)
    step, spot = place // quarter, lax.rem(place, quarter)

    z = 2 * side + step

    def device_at(floor, shift):
        return floor * quarter + lax.rem(spot + shift, quarter)

    def near_target(i):
        return device_at(2 * side + step, quarter - i)

    def cross_target(i):
        return device_at(2 * side + 1 - step, quarter - i)

    def far_target(i):
        return device_at(2 - 2 * side + lax.rem(i, 2), quarter - i // 2)

    def far_slot(i):
        return (1 + 2 * lax.rem(side + step, 2)) * quarter + i // 2

    def near_source(i):
        return device_at(2 * side + step, i)

    def outer_source(i):
        return device_at(3 - 3 * side, i)

    def cross_source(i):
        return device_at(2 * side + 1 - step, i)

    def inner_source(i):
        return device_at(2 - side, i)

    def slot_rows(i):
        return pl.ds(pl.multiple_of(i * cap, cap), cap)

    span = half * cap

    def buf_rows(j, i):
        return pl.ds(pl.multiple_of((i // half * peers + j) * span + lax.rem(i, half) * cap, cap), cap)

    barrier = pltpu.get_barrier_semaphore()

    def greet(target, j):
        pl.semaphore_signal(barrier, inc=1, device_id=(target, lax.rem(h + j, peers)), device_id_type=MESH)

    @pl.when(side == 0)
    def _():
        @pl.loop(1, n)
        def _(k):
            greet(lax.rem(b + k, n), 0)

        for j in range(1, peers):
            @pl.loop(0, quarter)
            def _(i):
                greet(near_target(i), j)

    @pl.when(z == 2)
    def _():
        for j in range(peers):
            @pl.loop(0, quarter)
            def _(i):
                greet(cross_target(i), j)

    loads = [
        pltpu.make_async_copy(source, target, local_sem.at[6 + at])
        for at, (source, target) in enumerate(
            [(x_hbm, pay.at[pl.ds(r * groups, groups), :, pl.ds(0, width)]) for r in range(n // groups)]
            + [(counts_hbm, counts_ref), (gate_hbm, gate_ref), (ids_hbm, ids_ref), (cot_hbm, cots)]
        )
    ]
    for load in loads:
        load.start()

    def call(k, target, j):
        pl.semaphore_signal(ready.at[k], inc=1, device_id=(target, lax.rem(h + j, peers)), device_id_type=MESH)

    @pl.when(z == 2)
    def _():
        pl.semaphore_wait(barrier, half)

        @pl.loop(0, half)
        def _(i):
            call(0, half - 1 - i, 0)

    @pl.when(z == 3)
    def _():
        pl.semaphore_wait(barrier, half + quarter * peers)

        @pl.loop(0, half)
        def _(i):
            call(1, i, 0)

        for j in range(peers):
            @pl.loop(0, quarter)
            def _(i):
                call(1, cross_target(i), j)

    get_w1 = pltpu.make_async_copy(w1_hbm.at[0], w1, local_sem.at[3])

    def get_w2(q):
        return pltpu.make_async_copy(w2_hbm.at[0, pl.ds(q * tile, tile)], w2.at[q % 2], turn_sem.at[q])

    get_w1.start()
    for q in range(2):
        get_w2(q).start()

    ahead = quarter // 2

    def far_part(i, part):
        target = far_target(i)
        columns = pl.ds(part * width, width)
        return pltpu.make_async_remote_copy(
            src_ref=pay.at[target, :, columns], dst_ref=buf.at[buf_rows(0, far_slot(i)), columns],
            send_sem=send1.at[1], recv_sem=recv1.at[far_slot(i)],
            device_id=(target, h), device_id_type=MESH,
        )

    for load in loads[:-4]:
        load.wait()

    @pl.when(z == 2)
    def _():
        @pl.loop(0, ahead)
        def _(i):
            far_part(i, 0).start()

    for load in loads[-4:]:
        load.wait()
    slots = groups * cap
    lanes = lax.broadcasted_iota(jnp.int32, (slots, slots), 1)
    places = lax.broadcasted_iota(jnp.int32, (slots, slots), 0)
    ids = jnp.broadcast_to(ids_ref[...].astype(jnp.float32), (slots, slots))
    tag[...] = jnp.broadcast_to(
        jnp.sum(jnp.where(lanes == places, ids, 0.0), axis=1, keepdims=True), tag.shape
    )
    order = lax.broadcasted_iota(jnp.int32, (cap, 1), 0)

    @pl.loop(0, groups)
    def _(g):
        known = tag[slot_rows(g), :][:, 0:1]
        live = order < counts_ref[0, g]
        cot_rows = cots[g].astype(jnp.float32)
        for r in range(n // groups):
            gate = jnp.zeros((cap, 1), jnp.float32)
            for t in range(tasks):
                gate = jnp.where(known == float(t), gate_ref[t, r * groups + g], gate)
            gate = jnp.where(live, gate, 0.0)
            pay[r * groups + g, :, pl.ds(width, width)] = (gate * cot_rows).astype(jnp.bfloat16)

    own = pltpu.make_async_copy(pay.at[b], buf.at[pl.ds(0, cap)], local_sem.at[2])
    own.start()

    def block_out(target, slot, kind=0):
        return pltpu.make_async_remote_copy(
            src_ref=pay.at[target], dst_ref=buf.at[buf_rows(0, slot)],
            send_sem=send1.at[kind], recv_sem=recv1.at[slot],
            device_id=(target, h), device_id_type=MESH,
        )

    def forward(i, j):
        return pltpu.make_async_remote_copy(
            src_ref=buf.at[buf_rows(0, i)], dst_ref=buf.at[buf_rows(j, i)],
            send_sem=send2.at[j - 1], recv_sem=recv2.at[j - 1, i // half],
            device_id=(b, lax.rem(h + j, peers)), device_id_type=MESH,
        )

    def across(i, j):
        target = near_target(i)
        return pltpu.make_async_remote_copy(
            src_ref=pay.at[target], dst_ref=buf.at[buf_rows(j, i)],
            send_sem=send2.at[j - 1], recv_sem=recv2.at[j - 1, i // half],
            device_id=(target, lax.rem(h + j, peers)), device_id_type=MESH,
        )

    def homeward(i, target):
        return pltpu.make_async_remote_copy(
            src_ref=ret.at[slot_rows(i)], dst_ref=home.at[b],
            send_sem=send3.at[0], recv_sem=recv3.at[0],
            device_id=(target, h), device_id_type=MESH,
        )

    def pass_on(i):
        block_out(b, i).wait_recv()
        for j in range(1, peers):
            forward(i, j).start()

    def send_far(start, stop, stride):
        @pl.loop(start, stop, step=stride)
        def _(i):
            block_out(far_target(i), far_slot(i), 1).start()

    def send_near():
        for j in range(1, peers):
            @pl.loop(0, quarter)
            def _(i):
                across(i, j).start()

        @pl.loop(1, quarter)
        def _(i):
            block_out(near_target(i), i).start()

    def send_cross():
        @pl.loop(0, quarter)
        def _(i):
            block_out(cross_target(i), half + i).start()

    @pl.when(side == 0)
    def _():
        pl.semaphore_wait(barrier, half - 1 + (peers - 1) * quarter)
        send_near()

        @pl.when(step == 1)
        def _():
            send_cross()

        pl.semaphore_wait(ready.at[0], quarter)
        send_far(0, quarter, 2)
        pl.semaphore_wait(ready.at[1], quarter)
        send_far(1, quarter, 2)
        send_far(quarter, half, 1)

        @pl.when(step == 0)
        def _():
            send_cross()

    @pl.when(z == 2)
    def _():
        @pl.loop(0, ahead)
        def _(i):
            far_part(i, 1).start()

        send_far(ahead, half, 1)
        pl.semaphore_wait(ready.at[1], quarter * peers)
        call(0, cross_target(0), 0)
        send_near()
        send_cross()

    @pl.when(z == 3)
    def _():
        send_far(0, half, 1)
        send_cross()
        pl.semaphore_wait(ready.at[0], 1)
        send_near()

    schedule = iter(SCHEDULE)

    def pick(values):
        value = values[0]
        for floor in range(1, 4):
            value = jnp.where(z == floor, values[floor], value)
        return value * quarter // 4

    def poll(wanted=True):
        if not wanted:
            return
        for ranges in next(schedule):
            @pl.loop(half + pick([start for start, _ in ranges]), half + pick([stop for _, stop in ranges]))
            def _(i):
                pass_on(i)

    get_w1.wait()
    for q in range(tiles):
        part = pl.ds(q * tile, tile)
        get_w2(q).wait()
        w2_turned[:, part] = w2[q % 2].T
        if q + 2 < tiles:
            get_w2(q + 2).start()
        w1_turned[part, :] = w1[:, part].T

    @pl.loop(quarter, half)
    def _(i):
        pass_on(i)

    poll()

    @pl.loop(1, quarter)
    def _(i):
        block_out(b, i).wait_recv()

    own.wait()

    def rows_forward(start, total, hook=lambda q: None):
        rows = pl.ds(start, total)

        def hidden_tile(q):
            at = lax.rem(h * hidden_part + q * tile, hidden)
            columns = pl.ds(pl.multiple_of(at, tile), tile)
            pre = jnp.dot(
                buf[rows, pl.ds(0, width)], w1[:, columns], preferred_element_type=jnp.float32
            )
            sig = jax.nn.sigmoid(pre)
            if q < part_tiles:
                act[rows, pl.ds(q * tile, tile)] = (pre * sig).astype(jnp.bfloat16)
            cot = jnp.dot(
                buf[rows, pl.ds(width, width)], w2_turned[:, columns], preferred_element_type=jnp.float32
            )
            pc[rows, columns] = (cot * (sig * (1.0 + pre * (1.0 - sig)))).astype(jnp.bfloat16)

        for q in range(tiles):
            hidden_tile(q)
            hook(q)

    def rows_home(part, hook=lambda d: None):
        rows = pl.ds(part * span, span)
        flat = pl.ds(part * peers * span, span)

        for d in range(width // tile):
            columns = pl.ds(d * tile, tile)
            grad = jnp.dot(pc[flat, :], w1_turned[:, columns], preferred_element_type=jnp.float32)
            ret[rows, columns] = grad.astype(jnp.bfloat16)
            hook(d)

    def partner_come(part):
        for j in range(1, peers):
            rows = buf.at[pl.ds((part * peers + j) * span, span)]
            pltpu.make_async_copy(rows, rows, recv2.at[j - 1, part]).wait()

    turned = (((0,), (0,)), ((), ()))
    chunk = peers * span

    def grads(part, hook=lambda: None):
        rows = pl.ds(part * chunk, chunk)

        def add(out, columns, left, right):
            grad = lax.dot_general(left, right, turned, preferred_element_type=jnp.float32)
            if part:
                grad = (out[:, columns] + grad) * grad_scale
            out[:, columns] = grad

        for q in range(tiles):
            columns = pl.ds(q * tile, tile)
            add(first, columns, buf[rows, pl.ds(pl.multiple_of(h * width_part, width_part), width_part)], pc[rows, columns])
        hook()
        for q in range(width // tile):
            columns = pl.ds(q * tile, tile)
            add(second, columns, act[rows, :], buf[rows, pl.ds(width + q * tile, tile)])

    outer = lax.rem(side + step, 2) == 0

    def far_sent():
        sent = pay.at[pl.ds(0, half)]
        pltpu.make_async_copy(sent, sent, send1.at[1]).wait()

    kept = quarter - (1 - side) * (quarter // 4)

    def send_back(base, source, start, stop):
        @pl.loop(start, stop)
        def _(t):
            i = base + lax.rem(t - spot + quarter, quarter)
            homeward(i, source(i)).start()

    def release(point):
        @pl.when(pick([4 * (point == chosen) for chosen in RELEASE]) > 0)
        def _():
            send_back(quarter, outer_source, 0, kept)

    def between():
        poll()
        release(1)

    rows_forward(0, span)
    poll()
    rows_home(0, lambda d: poll(d == 0))
    own_home = pltpu.make_async_copy(ret.at[pl.ds(0, cap)], home.at[b], local_sem.at[5])
    own_home.start()

    @pl.loop(1, quarter)
    def _(i):
        homeward(i, near_source(i)).start()

    poll()
    partner_come(0)
    rows_forward(span, chunk - span, lambda q: poll(2 * (q + 1) == tiles))
    poll()
    release(0)
    grads(0, between)

    @pl.when(jnp.logical_not(outer))
    def _():
        far_sent()
        send_back(quarter, outer_source, 0, kept)

    poll()

    release(2)

    rows_forward(chunk, span)
    rows_home(1)

    send_back(early, inner_source, 0, quarter)

    send_back(quarter, outer_source, kept, quarter)

    send_back(half, cross_source, 0, quarter)

    partner_come(1)
    rows_forward(chunk + span, chunk - span)

    grads(1)

    own_home.wait()

    sent = pay.at[pl.ds(0, half - 1)]
    pltpu.make_async_copy(sent, sent, send1.at[0]).wait()

    @pl.when(outer)
    def _():
        far_sent()

    for j in range(1, peers):
        whole = buf.at[pl.ds(0, 2 * span)]
        pltpu.make_async_copy(whole, whole, send2.at[j - 1]).wait()
    gone = ret.at[pl.ds(0, (n - 1) * cap)]
    pltpu.make_async_copy(gone, gone, send3.at[0]).wait()

    come = home.at[pl.ds(0, n - 1)]
    pltpu.make_async_copy(come, come, recv3.at[0]).wait()


def finish_kernel(first, second, home, out_rows, out_first, out_second, rows, sem):
    puts = []
    for source, target in ((first, out_first), (second, out_second)):
        step = source.shape[0] // PIECES
        for piece in range(PIECES):
            part = pl.ds(piece * step, step)
            puts.append(pltpu.make_async_copy(source.at[part], target.at[0, part], sem.at[len(puts)]))
            puts[-1].start()
    repeats, total = home.shape[0], jnp.float32(0.0)
    for r in range(repeats):
        total = total + home[r].astype(jnp.float32)
    rows[...] = total
    puts.append(pltpu.make_async_copy(rows, out_rows, sem.at[len(puts)]))
    puts[-1].start()
    for put in puts:
        put.wait()


def on_device(n, peers, inputs, cotangent, task_ids, group_counts, task_gate, w_in, w_out):
    groups = group_counts.shape[1]
    slots, width = inputs.shape
    hidden = w_in.shape[2]
    cap = slots // groups
    tasks = task_gate.shape[0]
    rows = peers * n * cap
    bf16 = jnp.bfloat16
    hbm = pl.BlockSpec(memory_space=pltpu.HBM)
    vmem = pl.BlockSpec(memory_space=pltpu.VMEM)
    dma = pltpu.SemaphoreType.DMA
    first, second, home = pl.pallas_call(
        functools.partial(exchange_kernel, n, peers, groups, cap, width, hidden, tasks),
        out_shape=(
            pltpu.VMEM((width // peers, hidden), jnp.float32),
            pltpu.VMEM((hidden // peers, width), jnp.float32),
            pltpu.VMEM((n, cap, width), bf16),
        ),
        in_specs=[hbm] * 7,
        out_specs=(vmem,) * 3,
        scratch_shapes=[
            pltpu.SMEM(group_counts.shape, jnp.int32),
            pltpu.SMEM(task_gate.shape, jnp.float32),
            pltpu.VMEM((1, slots), jnp.int32),
            pltpu.VMEM((groups, cap, width), bf16),
            pltpu.VMEM((slots, slots), jnp.float32),
            pltpu.VMEM((n, cap, 2 * width), bf16),
            pltpu.VMEM((rows, 2 * width), bf16),
            pltpu.VMEM((width, hidden), bf16),
            pltpu.VMEM((2, tile, width), bf16),
            pltpu.VMEM((hidden, width), bf16),
            pltpu.VMEM((width, hidden), bf16),
            pltpu.VMEM((n * cap, width), bf16),
            pltpu.VMEM((rows, hidden // peers), bf16),
            pltpu.VMEM((rows, hidden), bf16),
            dma((2,)), dma((n,)), dma((peers - 1,)), dma((peers - 1, 2)), dma((1,)), dma((1,)),
            dma((10 + n // groups,)),
            pltpu.SemaphoreType.REGULAR((2,)),
            dma((hidden // tile,)),
        ],
        compiler_params=pltpu.CompilerParams(
            collective_id=0, has_side_effects=True, vmem_limit_bytes=VMEM_BYTES
        ),
    )(
        *(
            pltpu.with_memory_space_constraint(array, pltpu.HBM)
            for array in (
                group_counts, task_gate, task_ids.reshape(1, slots), inputs.reshape(groups, cap, width),
                cotangent.reshape(groups, cap, width), w_in, w_out,
            )
        )
    )
    return pl.pallas_call(
        finish_kernel,
        out_shape=(
            jax.ShapeDtypeStruct((slots, width), jnp.float32),
            jax.ShapeDtypeStruct((1,) + first.shape, jnp.float32),
            jax.ShapeDtypeStruct((1,) + second.shape, jnp.float32),
        ),
        in_specs=[vmem] * 3,
        out_specs=(hbm,) * 3,
        scratch_shapes=[pltpu.VMEM((slots, width), jnp.float32), dma((2 * PIECES + 1,))],
        compiler_params=pltpu.CompilerParams(vmem_limit_bytes=4 * 1024 * 1024),
    )(first, second, home.reshape(n // groups, slots, width))


def solution(mesh):
    in_specs = (
        P(("blk", "dp"), None),
        P(("blk", "dp"), None),
        P(("blk", "dp")),
        P(("blk", "dp"), None),
        P(),
        P("blk", None, None),
        P("blk", None, None),
    )
    out_specs = (P(("blk", "dp"), None), P("blk", "dp", None), P("blk", "dp", None))
    body = functools.partial(on_device, mesh.shape["blk"], mesh.shape["dp"])
    return jax.shard_map(body, mesh=mesh, in_specs=in_specs, out_specs=out_specs, check_vma=False)
```

```python
import functools

import jax
import jax.numpy as jnp
from jax import lax
from jax.experimental import pallas as pl
from jax.experimental.pallas import tpu as pltpu
from jax.sharding import PartitionSpec as P

grad_scale = 0.0625
VMEM_BYTES = 51 * 1024 * 1024
PIECES = 4
RELEASE = (2, 9, 9, 1)
tile = 512
SCHEDULE = (
    (((0, 4), (0, 0), (0, 0), (0, 4)),),
    (((0, 0), (0, 1), (0, 0), (0, 0)),),
    (((0, 0), (1, 2), (0, 0), (0, 0)),),
    (((4, 6), (0, 0), (4, 6), (4, 5)),),
    (((0, 0), (2, 3), (0, 0), (0, 0)),),
    (((0, 0), (3, 6), (0, 2), (5, 6)),),
    (((6, 7), (6, 7), (0, 0), (6, 7)),),
    (((7, 8), (7, 8), (2, 4), (7, 8)), ((0, 0), (0, 0), (6, 8), (0, 0)),),
)
MESH = pl.DeviceIdType.MESH


def exchange_kernel(
    n, peers, groups, cap, width, hidden, tasks,
    counts_hbm, gate_hbm, ids_hbm, x_hbm, cot_hbm, w1_hbm, w2_hbm,
    first, second, home,
    counts_ref, gate_ref, ids_ref, cots, tag, pay, buf, w1, w2, w1_turned, w2_turned, ret, act, pc,
    send1, recv1, send2, recv2, send3, recv3, local_sem, ready, turn_sem,
):
    b = lax.axis_index("blk")
    h = lax.axis_index("dp")
    half, quarter = n // 2, n // 4
    early = n - quarter
    width_part = width // peers
    hidden_part = hidden // peers
    tiles = hidden // tile
    part_tiles = hidden_part // tile
    side, place = b // half, lax.rem(b, half)
    step, spot = place // quarter, lax.rem(place, quarter)

    z = 2 * side + step

    def device_at(floor, shift):
        return floor * quarter + lax.rem(spot + shift, quarter)

    def near_target(i):
        return device_at(2 * side + step, quarter - i)

    def cross_target(i):
        return device_at(2 * side + 1 - step, quarter - i)

    def far_target(i):
        return device_at(2 - 2 * side + lax.rem(i, 2), quarter - i // 2)

    def far_slot(i):
        return (1 + 2 * lax.rem(side + step, 2)) * quarter + i // 2

    def near_source(i):
        return device_at(2 * side + step, i)

    def outer_source(i):
        return device_at(3 - 3 * side, i)

    def cross_source(i):
        return device_at(2 * side + 1 - step, i)

    def inner_source(i):
        return device_at(2 - side, i)

    def slot_rows(i):
        return pl.ds(pl.multiple_of(i * cap, cap), cap)

    span = half * cap

    def buf_rows(j, i):
        return pl.ds(pl.multiple_of((i // half * peers + j) * span + lax.rem(i, half) * cap, cap), cap)

    barrier = pltpu.get_barrier_semaphore()

    def greet(target, j):
        pl.semaphore_signal(barrier, inc=1, device_id=(target, lax.rem(h + j, peers)), device_id_type=MESH)

    @pl.when(side == 0)
    def _():
        @pl.loop(1, n)
        def _(k):
            greet(lax.rem(b + k, n), 0)

        for j in range(1, peers):
            @pl.loop(0, quarter)
            def _(i):
                greet(near_target(i), j)

    @pl.when(z == 2)
    def _():
        for j in range(peers):
            @pl.loop(0, quarter)
            def _(i):
                greet(cross_target(i), j)

    loads = [
        pltpu.make_async_copy(source, target, local_sem.at[6 + at])
        for at, (source, target) in enumerate(
            [(x_hbm, pay.at[pl.ds(r * groups, groups), :, pl.ds(0, width)]) for r in range(n // groups)]
            + [(counts_hbm, counts_ref), (gate_hbm, gate_ref), (ids_hbm, ids_ref), (cot_hbm, cots)]
        )
    ]
    for load in loads:
        load.start()

    def call(k, target, j):
        pl.semaphore_signal(ready.at[k], inc=1, device_id=(target, lax.rem(h + j, peers)), device_id_type=MESH)

    @pl.when(z == 2)
    def _():
        pl.semaphore_wait(barrier, half)

        @pl.loop(0, half)
        def _(i):
            call(0, half - 1 - i, 0)

    @pl.when(z == 3)
    def _():
        pl.semaphore_wait(barrier, half + quarter * peers)

        @pl.loop(0, half)
        def _(i):
            call(1, i, 0)

        for j in range(peers):
            @pl.loop(0, quarter)
            def _(i):
                call(1, cross_target(i), j)

    get_w1 = pltpu.make_async_copy(w1_hbm.at[0], w1, local_sem.at[3])

    def get_w2(q):
        return pltpu.make_async_copy(w2_hbm.at[0, pl.ds(q * tile, tile)], w2.at[q % 2], turn_sem.at[q])

    get_w1.start()
    for q in range(2):
        get_w2(q).start()

    ahead = quarter // 2

    def far_part(i, part):
        target = far_target(i)
        columns = pl.ds(part * width, width)
        return pltpu.make_async_remote_copy(
            src_ref=pay.at[target, :, columns], dst_ref=buf.at[buf_rows(0, far_slot(i)), columns],
            send_sem=send1.at[1], recv_sem=recv1.at[far_slot(i)],
            device_id=(target, h), device_id_type=MESH,
        )

    for load in loads[:-4]:
        load.wait()

    @pl.when(z == 2)
    def _():
        @pl.loop(0, ahead)
        def _(i):
            far_part(i, 0).start()

    for load in loads[-4:]:
        load.wait()
    slots = groups * cap
    lanes = lax.broadcasted_iota(jnp.int32, (slots, slots), 1)
    places = lax.broadcasted_iota(jnp.int32, (slots, slots), 0)
    ids = jnp.broadcast_to(ids_ref[...].astype(jnp.float32), (slots, slots))
    tag[...] = jnp.broadcast_to(
        jnp.sum(jnp.where(lanes == places, ids, 0.0), axis=1, keepdims=True), tag.shape
    )
    order = lax.broadcasted_iota(jnp.int32, (cap, 1), 0)

    @pl.loop(0, groups)
    def _(g):
        known = tag[slot_rows(g), :][:, 0:1]
        live = order < counts_ref[0, g]
        cot_rows = cots[g].astype(jnp.float32)
        for r in range(n // groups):
            gate = jnp.zeros((cap, 1), jnp.float32)
            for t in range(tasks):
                gate = jnp.where(known == float(t), gate_ref[t, r * groups + g], gate)
            gate = jnp.where(live, gate, 0.0)
            pay[r * groups + g, :, pl.ds(width, width)] = (gate * cot_rows).astype(jnp.bfloat16)

    own = pltpu.make_async_copy(pay.at[b], buf.at[pl.ds(0, cap)], local_sem.at[2])
    own.start()

    def block_out(target, slot, kind=0):
        return pltpu.make_async_remote_copy(
            src_ref=pay.at[target], dst_ref=buf.at[buf_rows(0, slot)],
            send_sem=send1.at[kind], recv_sem=recv1.at[slot],
            device_id=(target, h), device_id_type=MESH,
        )

    def forward(i, j):
        return pltpu.make_async_remote_copy(
            src_ref=buf.at[buf_rows(0, i)], dst_ref=buf.at[buf_rows(j, i)],
            send_sem=send2.at[j - 1], recv_sem=recv2.at[j - 1, i // half],
            device_id=(b, lax.rem(h + j, peers)), device_id_type=MESH,
        )

    def across(i, j):
        target = near_target(i)
        return pltpu.make_async_remote_copy(
            src_ref=pay.at[target], dst_ref=buf.at[buf_rows(j, i)],
            send_sem=send2.at[j - 1], recv_sem=recv2.at[j - 1, i // half],
            device_id=(target, lax.rem(h + j, peers)), device_id_type=MESH,
        )

    def homeward(i, target):
        return pltpu.make_async_remote_copy(
            src_ref=ret.at[slot_rows(i)], dst_ref=home.at[b],
            send_sem=send3.at[0], recv_sem=recv3.at[0],
            device_id=(target, h), device_id_type=MESH,
        )

    def pass_on(i):
        block_out(b, i).wait_recv()
        for j in range(1, peers):
            forward(i, j).start()

    def send_far(start, stop, stride):
        @pl.loop(start, stop, step=stride)
        def _(i):
            block_out(far_target(i), far_slot(i), 1).start()

    def send_near():
        for j in range(1, peers):
            @pl.loop(0, quarter)
            def _(i):
                across(i, j).start()

        @pl.loop(1, quarter)
        def _(i):
            block_out(near_target(i), i).start()

    def send_cross():
        @pl.loop(0, quarter)
        def _(i):
            block_out(cross_target(i), half + i).start()

    @pl.when(side == 0)
    def _():
        pl.semaphore_wait(barrier, half - 1 + (peers - 1) * quarter)
        send_near()

        @pl.when(step == 1)
        def _():
            send_cross()

        pl.semaphore_wait(ready.at[0], quarter)
        send_far(0, quarter, 2)
        pl.semaphore_wait(ready.at[1], quarter)
        send_far(1, quarter, 2)
        send_far(quarter, half, 1)

        @pl.when(step == 0)
        def _():
            send_cross()

    @pl.when(z == 2)
    def _():
        @pl.loop(0, ahead)
        def _(i):
            far_part(i, 1).start()

        send_far(ahead, half, 1)
        pl.semaphore_wait(ready.at[1], quarter * peers)
        call(0, cross_target(0), 0)
        send_near()
        send_cross()

    @pl.when(z == 3)
    def _():
        send_far(0, half, 1)
        send_cross()
        pl.semaphore_wait(ready.at[0], 1)
        send_near()

    schedule = iter(SCHEDULE)

    def pick(values):
        value = values[0]
        for floor in range(1, 4):
            value = jnp.where(z == floor, values[floor], value)
        return value * quarter // 4

    def poll(wanted=True):
        if not wanted:
            return
        for ranges in next(schedule):
            @pl.loop(half + pick([start for start, _ in ranges]), half + pick([stop for _, stop in ranges]))
            def _(i):
                pass_on(i)

    get_w1.wait()
    for q in range(tiles):
        part = pl.ds(q * tile, tile)
        get_w2(q).wait()
        w2_turned[:, part] = w2[q % 2].T
        if q + 2 < tiles:
            get_w2(q + 2).start()
        w1_turned[part, :] = w1[:, part].T

    @pl.loop(quarter, half)
    def _(i):
        pass_on(i)

    poll()

    @pl.loop(1, quarter)
    def _(i):
        block_out(b, i).wait_recv()

    own.wait()

    def rows_forward(start, total, hook=lambda q: None):
        rows = pl.ds(start, total)

        def hidden_tile(q):
            at = lax.rem(h * hidden_part + q * tile, hidden)
            columns = pl.ds(pl.multiple_of(at, tile), tile)
            pre = jnp.dot(
                buf[rows, pl.ds(0, width)], w1[:, columns], preferred_element_type=jnp.float32
            )
            sig = jax.nn.sigmoid(pre)
            if q < part_tiles:
                act[rows, pl.ds(q * tile, tile)] = (pre * sig).astype(jnp.bfloat16)
            cot = jnp.dot(
                buf[rows, pl.ds(width, width)], w2_turned[:, columns], preferred_element_type=jnp.float32
            )
            pc[rows, columns] = (cot * (sig * (1.0 + pre * (1.0 - sig)))).astype(jnp.bfloat16)

        for q in range(tiles):
            hidden_tile(q)
            hook(q)

    def rows_home(part, hook=lambda d: None):
        rows = pl.ds(part * span, span)
        flat = pl.ds(part * peers * span, span)

        for d in range(width // tile):
            columns = pl.ds(d * tile, tile)
            grad = jnp.dot(pc[flat, :], w1_turned[:, columns], preferred_element_type=jnp.float32)
            ret[rows, columns] = grad.astype(jnp.bfloat16)
            hook(d)

    def partner_come(part):
        for j in range(1, peers):
            rows = buf.at[pl.ds((part * peers + j) * span, span)]
            pltpu.make_async_copy(rows, rows, recv2.at[j - 1, part]).wait()

    turned = (((0,), (0,)), ((), ()))
    chunk = peers * span

    def grads(part, hook=lambda: None):
        rows = pl.ds(part * chunk, chunk)

        def add(out, columns, left, right):
            grad = lax.dot_general(left, right, turned, preferred_element_type=jnp.float32)
            if part:
                grad = (out[:, columns] + grad) * grad_scale
            out[:, columns] = grad

        for q in range(tiles):
            columns = pl.ds(q * tile, tile)
            add(first, columns, buf[rows, pl.ds(pl.multiple_of(h * width_part, width_part), width_part)], pc[rows, columns])
        hook()
        for q in range(width // tile):
            columns = pl.ds(q * tile, tile)
            add(second, columns, act[rows, :], buf[rows, pl.ds(width + q * tile, tile)])

    outer = lax.rem(side + step, 2) == 0

    def far_sent():
        sent = pay.at[pl.ds(0, half)]
        pltpu.make_async_copy(sent, sent, send1.at[1]).wait()

    kept = quarter - (1 - side) * step * (quarter // 4)

    def send_back(base, source, start, stop):
        @pl.loop(start, stop)
        def _(at):
            turned_back = at // (quarter // 2) * lax.rem(spot, 2)
            t = at + turned_back * (quarter + quarter // 2 - 1 - 2 * at)
            i = base + lax.rem(t - spot + quarter, quarter)
            homeward(i, source(i)).start()

    def release(point):
        @pl.when(pick([4 * (point == chosen) for chosen in RELEASE]) > 0)
        def _():
            send_back(quarter, outer_source, 0, kept)

    def between():
        poll()
        release(1)

    rows_forward(0, span)
    poll()
    rows_home(0, lambda d: poll(d == 0))
    own_home = pltpu.make_async_copy(ret.at[pl.ds(0, cap)], home.at[b], local_sem.at[5])
    own_home.start()

    @pl.loop(1, quarter)
    def _(i):
        homeward(i, near_source(i)).start()

    poll()
    partner_come(0)
    rows_forward(span, chunk - span, lambda q: poll(2 * (q + 1) == tiles))
    poll()
    release(0)
    grads(0, between)

    @pl.when(jnp.logical_not(outer))
    def _():
        far_sent()
        send_back(quarter, outer_source, 0, kept)

    poll()

    release(2)

    rows_forward(chunk, span)
    rows_home(1)

    send_back(early, inner_source, 0, quarter)

    send_back(quarter, outer_source, kept, quarter)

    send_back(half, cross_source, 0, quarter)

    partner_come(1)
    rows_forward(chunk + span, chunk - span)

    grads(1)

    own_home.wait()

    sent = pay.at[pl.ds(0, half - 1)]
    pltpu.make_async_copy(sent, sent, send1.at[0]).wait()

    @pl.when(outer)
    def _():
        far_sent()

    for j in range(1, peers):
        whole = buf.at[pl.ds(0, 2 * span)]
        pltpu.make_async_copy(whole, whole, send2.at[j - 1]).wait()
    gone = ret.at[pl.ds(0, (n - 1) * cap)]
    pltpu.make_async_copy(gone, gone, send3.at[0]).wait()

    come = home.at[pl.ds(0, n - 1)]
    pltpu.make_async_copy(come, come, recv3.at[0]).wait()


def finish_kernel(first, second, home, out_rows, out_first, out_second, rows, sem):
    puts = []
    for source, target in ((first, out_first), (second, out_second)):
        step = source.shape[0] // PIECES
        for piece in range(PIECES):
            part = pl.ds(piece * step, step)
            puts.append(pltpu.make_async_copy(source.at[part], target.at[0, part], sem.at[len(puts)]))
            puts[-1].start()
    repeats, total = home.shape[0], jnp.float32(0.0)
    for r in range(repeats):
        total = total + home[r].astype(jnp.float32)
    rows[...] = total
    puts.append(pltpu.make_async_copy(rows, out_rows, sem.at[len(puts)]))
    puts[-1].start()
    for put in puts:
        put.wait()


def on_device(n, peers, inputs, cotangent, task_ids, group_counts, task_gate, w_in, w_out):
    groups = group_counts.shape[1]
    slots, width = inputs.shape
    hidden = w_in.shape[2]
    cap = slots // groups
    tasks = task_gate.shape[0]
    rows = peers * n * cap
    bf16 = jnp.bfloat16
    hbm = pl.BlockSpec(memory_space=pltpu.HBM)
    vmem = pl.BlockSpec(memory_space=pltpu.VMEM)
    dma = pltpu.SemaphoreType.DMA
    first, second, home = pl.pallas_call(
        functools.partial(exchange_kernel, n, peers, groups, cap, width, hidden, tasks),
        out_shape=(
            pltpu.VMEM((width // peers, hidden), jnp.float32),
            pltpu.VMEM((hidden // peers, width), jnp.float32),
            pltpu.VMEM((n, cap, width), bf16),
        ),
        in_specs=[hbm] * 7,
        out_specs=(vmem,) * 3,
        scratch_shapes=[
            pltpu.SMEM(group_counts.shape, jnp.int32),
            pltpu.SMEM(task_gate.shape, jnp.float32),
            pltpu.VMEM((1, slots), jnp.int32),
            pltpu.VMEM((groups, cap, width), bf16),
            pltpu.VMEM((slots, slots), jnp.float32),
            pltpu.VMEM((n, cap, 2 * width), bf16),
            pltpu.VMEM((rows, 2 * width), bf16),
            pltpu.VMEM((width, hidden), bf16),
            pltpu.VMEM((2, tile, width), bf16),
            pltpu.VMEM((hidden, width), bf16),
            pltpu.VMEM((width, hidden), bf16),
            pltpu.VMEM((n * cap, width), bf16),
            pltpu.VMEM((rows, hidden // peers), bf16),
            pltpu.VMEM((rows, hidden), bf16),
            dma((2,)), dma((n,)), dma((peers - 1,)), dma((peers - 1, 2)), dma((1,)), dma((1,)),
            dma((10 + n // groups,)),
            pltpu.SemaphoreType.REGULAR((2,)),
            dma((hidden // tile,)),
        ],
        compiler_params=pltpu.CompilerParams(
            collective_id=0, has_side_effects=True, vmem_limit_bytes=VMEM_BYTES
        ),
    )(
        *(
            pltpu.with_memory_space_constraint(array, pltpu.HBM)
            for array in (
                group_counts, task_gate, task_ids.reshape(1, slots), inputs.reshape(groups, cap, width),
                cotangent.reshape(groups, cap, width), w_in, w_out,
            )
        )
    )
    return pl.pallas_call(
        finish_kernel,
        out_shape=(
            jax.ShapeDtypeStruct((slots, width), jnp.float32),
            jax.ShapeDtypeStruct((1,) + first.shape, jnp.float32),
            jax.ShapeDtypeStruct((1,) + second.shape, jnp.float32),
        ),
        in_specs=[vmem] * 3,
        out_specs=(hbm,) * 3,
        scratch_shapes=[pltpu.VMEM((slots, width), jnp.float32), dma((2 * PIECES + 1,))],
        compiler_params=pltpu.CompilerParams(vmem_limit_bytes=4 * 1024 * 1024),
    )(first, second, home.reshape(n // groups, slots, width))


def solution(mesh):
    in_specs = (
        P(("blk", "dp"), None),
        P(("blk", "dp"), None),
        P(("blk", "dp")),
        P(("blk", "dp"), None),
        P(),
        P("blk", None, None),
        P("blk", None, None),
    )
    out_specs = (P(("blk", "dp"), None), P("blk", "dp", None), P("blk", "dp", None))
    body = functools.partial(on_device, mesh.shape["blk"], mesh.shape["dp"])
    return jax.shard_map(body, mesh=mesh, in_specs=in_specs, out_specs=out_specs, check_vma=False)
```
